128 devices in a mesh: slab: 32 (over z, y, core), plane: 4 (over x).
Axes of the slice: x: 4, y: 4, z: 4, core: 2. Of those that a mesh axis runs over, the one named last changes fastest.
Arguments:
- tissue_v: float32 [128, 64, 128], P('slab', 'plane'), may hold values from -4 to 4
- tissue_gates: float32 [40, 128, 64, 128], P(None, 'slab', 'plane'), may hold values from 0 to 1
- tissue_diff: float32 [128, 64, 128], P('slab', 'plane'), may hold values from 0.2 to 1
- fibre_v: float32 [512, 2048], P('slab', 'plane'), may hold values from -4 to 4
- fibre_gates: float32 [40, 512, 2048], P(None, 'slab', 'plane'), may hold values from 0 to 1
- fibre_diff: float32 [512, 2048], P('slab', 'plane'), may hold values from 0.2 to 1
- gate_half: float32 [40], replicated, may hold values from -3 to 3
- gate_rate: float32 [40], replicated, may hold values from 0.5 to 20
- gate_cond: float32 [40], replicated, may hold values from 0.01 to 0.15
- gate_rev: float32 [40], replicated, may hold values from -2 to 2
- junc_cond: float32 [8], replicated, may hold values from 0.25 to 2
- junc_fibre: int32 [524288], P(('slab', 'plane')), may hold values from 0 to 15
- junc_fcell: int32 [524288], P(('slab', 'plane')), may hold values from 0 to 511
- junc_owner: int32 [524288, 1], P(('slab', 'plane')), may hold values from 0 to 127; in each aligned block of 4096 rows (0 to 4095, 4096 to 8191, ...) at most 64 rows name the same one
- junc_tcell: int32 [524288], P(('slab', 'plane')), may hold values from 0 to 8191
- junc_class: int32 [524288], P(('slab', 'plane')), may hold values from 0 to 7
Outputs:
- tissue_out: float32 [128, 64, 128], P('slab', 'plane')
- fibre_out: float32 [512, 2048], P('slab', 'plane')
The draws below stay inside these ranges and needn't reach their ends.
Inputs may be any that keep to these rules, and one draw needn't show every extreme that they name: `junc_owner`: among the junctions held by one device, no tissue block is named by more than 64 of them, and some block is named by exactly 64. `junc_fibre`: A fibre of the slab group of the device that holds the junction. `junc_fcell`: A cell of the holding device's share of that fibre. `junc_tcell`: numbered over the owner's block in the order z, y, x with x fastest.
All inputs are finite; a program needn't handle non-finite values.
Results may differ from the reference program's by a relative error of at most 0.00005.
Values sent between devices are 32-bit elements; how exact they have to be, the bound alone decides.
A program may use at most 64 MiB of HBM per device.

```python
import math
import jax
import jax.numpy as jnp
import numpy as np
from jax import lax

NX = 128
CY = 16
CZ = 4
FIB_DEV = 16
FCELLS = 2048
GATES = 40
CLASSES = 8
STEPS = 14
JUNC_DEV = 4096
CAP = 64
NZ = 128
NY = 64
NFIB = 512
JUNCS = 524288
N_PLANE = 4
DEVICES = 128


def set_ends(result, own_key, least, high):
    dims = result.shape
    index_at = [jax.random.randint(jax.random.fold_in(own_key, axis), (), 0, dims[axis]) for axis in range(len(dims))]
    result = result.at[tuple(index_at)].set(least)
    longest = dims.index(max(dims))
    index_at[longest] = (index_at[longest] + 1) % dims[longest]
    return result.at[tuple(index_at)].set(high)


def block_scale(rng, dims, pieces, smallest, largest):
    gain, own = 1.0, jax.random.fold_in(rng, 6)
    for axis_at, blocks in pieces:
        draws = jnp.exp(jax.random.uniform(jax.random.fold_in(own, axis_at), (blocks,), jnp.float32, smallest / len(pieces), largest / len(pieces)))
        gain = gain * jnp.repeat(draws, dims[axis_at] // blocks).reshape([-1 if axis == axis_at else 1 for axis in range(len(dims))])
    return gain


def shared_out(rng, own, number, rows, amount, top, reach, lean):
    ranking = jax.random.permutation(rng, amount)
    packed, usual = shares(amount, rows * top, reach, lean, True), shares(amount, rows * top, reach, lean, False)
    places = jnp.arange(amount)

    def named(sizes, rotation):
        used = int((sizes > 0).sum())
        fixed = max(1, used // 4)
        moved = fixed + (places - fixed + rotation * (used - fixed)) % max(1, amount - fixed)
        return jnp.zeros((amount,), jnp.int32).at[ranking[jnp.where(places < fixed, places, moved)]].set(jnp.asarray(sizes, jnp.int32))

    sizes = jnp.where(number % 4 == 0, named(packed, number // 4), named(usual, number - number // 4 - 1))
    mixed = jax.random.permutation(jax.random.fold_in(own, 3), amount)
    giver, sink = mixed[0:amount // 2 * 2:2], mixed[1:amount // 2 * 2:2]
    room = jnp.minimum(sizes[giver] - 1, reach - sizes[sink]) // 2
    room = jnp.where((giver == ranking[0]) | (sink == ranking[0]) | (sizes[sink] == 0), 0, jnp.maximum(room, 0))
    moved = jax.random.randint(jax.random.fold_in(own, 4), (amount // 2,), 0, 1 << 20) % (room + 1)
    sizes = sizes.at[giver].add(-moved).at[sink].add(moved)
    items = jnp.searchsorted(jnp.cumsum(sizes), jnp.arange(rows * top), side="right").astype(jnp.int32)
    table = items.reshape(top, rows).T
    table = table[jax.random.permutation(jax.random.fold_in(own, 1), rows)]
    rotation = jax.random.randint(jax.random.fold_in(own, 2), (rows, 1), 0, top)
    return jnp.take_along_axis(table, (jnp.arange(top)[None, :] + rotation) % top, axis=1)


def shares(count, total, limit, lean, full):
    loads = [(1 << 20) // math.isqrt(grade ** lean) + 1 for grade in range(1, count + 1)]
    largest = limit if full else min(limit, max(-(-total // count), total * loads[0] // sum(loads)))
    least = 1 if total - largest >= count - 1 else 0
    holding, surplus = [largest] + [least] * (count - 1), total - largest - least * (count - 1)
    while surplus > 0:
        candidates = [i for i in range(1, count) if holding[i] < largest] or [i for i in range(1, count) if holding[i] < limit]
        mass, remaining = sum([loads[i] for i in candidates]), surplus
        for i in candidates:
            extra = min(limit - holding[i], max(1, remaining * loads[i] // mass), surplus)
            holding[i] = holding[i] + extra
            surplus = surplus - extra
    return np.array(holding)


def centred(rng, shape, scale, bound, split=(), kind=jnp.bfloat16):
    drawn = jax.random.normal(rng, shape, jnp.float32) * scale
    if len(split) > 0:
        drawn = block_scale(rng, shape, split, -0.22, 0.18) * drawn
    return jnp.clip(drawn, min=-bound, max=bound).astype(kind)


def setup_inputs(seed: int = 0) -> dict:
    splits = jax.random.split(jax.random.key(seed), 17)
    tissue_v = centred(splits[0], (NZ, NY, NX), 1.0, 4.0, ((0, 32), (1, 4)), jnp.float32)
    tissue_gates = jnp.clip(1.0 * jax.random.uniform(splits[1], (GATES, NZ, NY, NX), jnp.float32) ** block_scale(splits[1], (GATES, NZ, NY, NX), ((1, 32), (2, 4)), -0.2, 0.2), 0.0, 1.0)
    tissue_diff = jnp.clip(jnp.exp(math.log(1.0) - 1.609438 * jax.random.uniform(splits[2], (NZ, NY, NX), jnp.float32) ** block_scale(splits[2], (NZ, NY, NX), ((0, 32), (1, 4)), -0.2, 0.2)), 0.2, 1.0)
    fibre_v = centred(splits[3], (NFIB, FCELLS), 1.0, 4.0, ((0, 32), (1, 4)), jnp.float32)
    fibre_gates = jnp.clip(1.0 * jax.random.uniform(splits[4], (GATES, NFIB, FCELLS), jnp.float32) ** block_scale(splits[4], (GATES, NFIB, FCELLS), ((1, 32), (2, 4)), -0.2, 0.2), 0.0, 1.0)
    fibre_diff = jnp.clip(jnp.exp(math.log(1.0) - 1.609438 * jax.random.uniform(splits[5], (NFIB, FCELLS), jnp.float32) ** block_scale(splits[5], (NFIB, FCELLS), ((0, 32), (1, 4)), -0.2, 0.2)), 0.2, 1.0)
    gate_half = centred(splits[6], (GATES,), 1.0, 3.0, (), jnp.float32)
    gate_rate = jnp.clip(jnp.exp(jax.random.uniform(splits[7], (GATES,), jnp.float32, math.log(0.5), math.log(20.0))), 0.5, 20.0)
    gate_cond = jnp.clip(jnp.exp(jax.random.uniform(splits[8], (GATES,), jnp.float32, math.log(0.01), math.log(0.15))), 0.01, 0.15)
    gate_rev = jnp.clip(jax.random.uniform(splits[9], (GATES,), jnp.float32, -2.0, 2.0), -2.0, 2.0)
    junc_cond = jnp.clip(jnp.exp(jax.random.uniform(splits[10], (CLASSES,), jnp.float32, math.log(0.25), math.log(2.0))), 0.25, 2.0)
    junc_fibre = set_ends(jax.random.randint(splits[11], (JUNCS,), 0, FIB_DEV), jax.random.fold_in(splits[11], 1), 0, FIB_DEV - 1).astype(jnp.int32)
    junc_fcell = set_ends(jax.random.randint(splits[12], (JUNCS,), 0, FCELLS // N_PLANE), jax.random.fold_in(splits[12], 1), 0, (FCELLS // N_PLANE) - 1).astype(jnp.int32)
    junc_owner_keys = jax.random.split(jax.random.fold_in(splits[13], 1), JUNCS // JUNC_DEV)
    junc_owner_turns = jax.random.permutation(jax.random.fold_in(splits[13], 3), JUNCS // JUNC_DEV)
    junc_owner = jax.vmap(lambda own, number: shared_out(jax.random.fold_in(splits[13], 2), own, number, JUNC_DEV, DEVICES, 1, CAP, 2))(junc_owner_keys, junc_owner_turns).reshape((JUNCS, 1))
    junc_tcell = set_ends(jax.random.randint(splits[14], (JUNCS,), 0, CZ * CY * NX), jax.random.fold_in(splits[14], 1), 0, (CZ * CY * NX) - 1).astype(jnp.int32)
    junc_class = set_ends(jax.random.randint(splits[15], (JUNCS,), 0, CLASSES), jax.random.fold_in(splits[15], 1), 0, CLASSES - 1).astype(jnp.int32)
    return {"tissue_v": tissue_v, "tissue_gates": tissue_gates, "tissue_diff": tissue_diff, "fibre_v": fibre_v, "fibre_gates": fibre_gates, "fibre_diff": fibre_diff, "gate_half": gate_half, "gate_rate": gate_rate, "gate_cond": gate_cond, "gate_rev": gate_rev, "junc_cond": junc_cond, "junc_fibre": junc_fibre, "junc_fcell": junc_fcell, "junc_owner": junc_owner, "junc_tcell": junc_tcell, "junc_class": junc_class}


time_step = 0.1
gate_slope = 2.0


def membrane(voltage, gates, gate_half, gate_rate, gate_cond, gate_rev):
    gate_signs = jnp.where(jnp.arange(GATES, dtype=jnp.int32) % 2 == 0, 1.0, -1.0).astype(jnp.float32)

    def one_gate(totals, inputs):
        gate_now, mid_point, speed, conductance, reversal, direction = inputs
        shifted = voltage - mid_point
        steady = jax.nn.sigmoid(direction * gate_slope * shifted)
        decay_factor = jnp.exp(-time_step * speed * (1.0 + jax.nn.sigmoid(shifted)))
        renewed = steady + (gate_now - steady) * decay_factor
        return (totals[0] + conductance * renewed, totals[1] + (conductance * reversal) * renewed), renewed

    zero_field = jnp.zeros_like(voltage)
    sums, renewed_all = lax.scan(one_gate, (zero_field, zero_field), (gates, gate_half, gate_rate, gate_cond, gate_rev, gate_signs))
    ionic = voltage * sums[0] - sums[1]
    return renewed_all, ionic


def line_count(length):
    places = jnp.arange(length, dtype=jnp.int32)
    return (places > 0).astype(jnp.float32) + (places < length - 1).astype(jnp.float32)


def reference(tissue_v, tissue_gates, tissue_diff, fibre_v, fibre_gates, fibre_diff, gate_half, gate_rate, gate_cond, gate_rev, junc_cond, junc_fibre, junc_fcell, junc_owner, junc_tcell, junc_class):
    depth_all, height_all, width_all = tissue_v.shape
    fibre_total, fibre_len = fibre_v.shape
    share = fibre_len // N_PLANE
    total_junctions = junc_fibre.shape[0]
    holder = jnp.arange(total_junctions, dtype=jnp.int32) // JUNC_DEV
    fibre_row = (holder // N_PLANE) * FIB_DEV + junc_fibre
    fibre_col = (holder % N_PLANE) * share + junc_fcell
    fibre_flat = (fibre_row * fibre_len + fibre_col).astype(jnp.int32)
    owners = junc_owner[:, 0]
    layer_z = (owners // N_PLANE) * CZ + junc_tcell // (CY * NX)
    row_y = (owners % N_PLANE) * CY + (junc_tcell // NX) % CY
    tissue_flat = ((layer_z * height_all + row_y) * width_all + junc_tcell % NX).astype(jnp.int32)
    coupling = jnp.sum(jnp.where(junc_class[:, None] == jnp.arange(CLASSES, dtype=jnp.int32)[None, :], junc_cond[None, :], jnp.zeros((), jnp.float32)), axis=1)
    tissue_count = line_count(depth_all)[:, None, None] + line_count(height_all)[None, :, None] + line_count(width_all)[None, None, :]
    fibre_count = line_count(fibre_len)[None, :]

    def advance(carry, unused):
        tissue_now, tissue_state, fibre_now, fibre_state = carry
        tissue_line = tissue_now.reshape(-1)
        fibre_line = fibre_now.reshape(-1)
        current = coupling * (fibre_line[fibre_flat] - tissue_line[tissue_flat])
        tissue_source = jnp.zeros_like(tissue_line).at[tissue_flat].add(current).reshape(tissue_now.shape)
        fibre_source = jnp.zeros_like(fibre_line).at[fibre_flat].add(-current).reshape(fibre_now.shape)
        padded = jnp.pad(tissue_now, 1)
        neighbours = padded[2:, 1:-1, 1:-1] + padded[:-2, 1:-1, 1:-1] + padded[1:-1, 2:, 1:-1] + padded[1:-1, :-2, 1:-1] + padded[1:-1, 1:-1, 2:] + padded[1:-1, 1:-1, :-2]
        tissue_lap = neighbours - tissue_count * tissue_now
        fibre_padded = jnp.pad(fibre_now, ((0, 0), (1, 1)))
        fibre_lap = fibre_padded[:, 2:] + fibre_padded[:, :-2] - fibre_count * fibre_now
        tissue_state, tissue_ionic = membrane(tissue_now, tissue_state, gate_half, gate_rate, gate_cond, gate_rev)
        fibre_state, fibre_ionic = membrane(fibre_now, fibre_state, gate_half, gate_rate, gate_cond, gate_rev)
        tissue_next = tissue_now + time_step * (tissue_diff * tissue_lap - tissue_ionic + tissue_source)
        fibre_next = fibre_now + time_step * (fibre_diff * fibre_lap - fibre_ionic + fibre_source)
        return (tissue_next, tissue_state, fibre_next, fibre_state), None

    final, unused_out = lax.scan(advance, (tissue_v, tissue_gates, fibre_v, fibre_gates), None, length=STEPS)
    return final[0], final[2]
```

```python
import functools

import jax
import jax.numpy as jnp
from jax import lax
from jax.experimental import pallas as pl
from jax.experimental.pallas import tpu as pltpu
from jax.sharding import PartitionSpec as P

STEPS = 14
DT = 0.1
LOG2E = 1.4426950408889634
MESH = pl.DeviceIdType.MESH
f32, bf16, i32 = jnp.float32, jnp.bfloat16, jnp.int32


def offsets():
    ring = lambda d: min(d, 4 - d)
    every = [(a, b, c, d) for a in range(4) for b in range(4) for c in range(2) for d in range(4)]
    far = lambda o: ring(o[0]) + ring(o[1]) + ring(o[3]) + 0.1 * o[2]
    return sorted([o for o in every if any(o)], key=lambda o: -far(o))


def iota(shape, dim):
    return lax.broadcasted_iota(i32, shape, dim)


def kernel(
    tv_ref, td_ref, fv_ref, fd_ref, tg_ref, fg_ref,
    half_ref, rate_ref, cond_ref, rev_ref, jcond_ref,
    jf_ref, jc_ref, jo_ref, jt_ref, jk_ref,
    to_ref, fo_ref,
    v_ref, d_ref, y_ref, prm_ref,
    oht_ref, kv_ref, rmask_ref, ct_ref, c_ref,
    row_ref, lane_ref, gain_ref, gsum_ref, graw_ref,
    s0_ref, r0_ref, s_ref, r_ref, hb_ref, hy_ref,
    gsem, s0sem, r0sem, ssem, rsem, hssem, hrsem,
):
    slab, plane = lax.axis_index("slab"), lax.axis_index("plane")
    me = slab * 4 + plane
    z, y, core = slab // 8, lax.rem(slab // 2, 4), lax.rem(slab, 2)
    half = me // 64
    q_me = lax.rem(me, 64)
    zs = [lax.rem(z + d, 4) * 8 for d in range(4)]
    ys = [lax.rem(y + d, 4) * 2 for d in range(4)]
    cs = [lax.rem(core + d, 2) for d in range(2)]
    xs = [lax.rem(plane + d, 4) for d in range(4)]
    peers = [(zs[a] + ys[b] + cs[c], xs[d]) for a, b, c, d in offsets()]

    loads = [pltpu.make_async_copy(tg_ref, y_ref.at[0], gsem.at[0])]
    for t in range(4):
        loads.append(pltpu.make_async_copy(fg_ref.at[:, :, pl.ds(t * 128, 128)], y_ref.at[1, :, t], gsem.at[1 + t]))
    for copy in loads:
        copy.start()

    barrier = pltpu.get_barrier_semaphore()

    def greet(k, carry):
        t = lax.rem(me + k, 128)
        pl.semaphore_signal(barrier, inc=1, device_id=(t // 4, lax.rem(t, 4)), device_id_type=MESH)
        return carry

    lax.fori_loop(1, 128, greet, 0)

    def params(k, carry):
        rate, cond = rate_ref[k], cond_ref[k]
        prm_ref[0, k] = 0.5 * half_ref[k]
        prm_ref[1, k] = rate * (-1.5 * DT * LOG2E)
        prm_ref[2, k] = rate * (-0.5 * DT * LOG2E)
        prm_ref[3, k] = 0.5 * cond
        prm_ref[4, k] = rev_ref[k]
        prm_ref[5, k] = cond
        return carry

    lax.fori_loop(0, 40, params, 0)

    v_ref[0, 0] = tv_ref[...]
    d_ref[0] = td_ref[...]
    for t in range(4):
        v_ref[1, 0, t] = fv_ref[:, t * 128:(t + 1) * 128]
        d_ref[1, t] = fd_ref[:, t * 128:(t + 1) * 128]

    sub = iota((128, 128), 0)
    sub64 = iota((64, 128), 0)
    lane = iota((128, 128), 1)
    lane64 = iota((64, 128), 1)
    before = jnp.concatenate([jnp.where(sub < lane, 1.0, 0.0), jnp.ones((128, 128), f32)], axis=1).astype(bf16)

    def chunk(c, count):
        at = pl.ds(c, 1)
        cols = pl.ds(pl.multiple_of(c * 128, 128), 128)
        hit = sub == jnp.broadcast_to(jo_ref[at, :], (128, 128))
        onehot = jnp.where(hit, 1.0, 0.0).astype(bf16)
        oht_ref[:, cols] = onehot
        seen = jnp.dot(onehot, before, preferred_element_type=f32)
        rank = jnp.sum(jnp.where(hit, seen[:, :128] + count, 0.0), axis=0, keepdims=True).astype(i32)
        place = sub64 == jnp.broadcast_to(rank, (64, 128))

        def put(p, value):
            value = jnp.broadcast_to(value.astype(f32), (64, 128))
            kv_ref[p * 64:(p + 1) * 64, cols] = jnp.where(place, value, 0.0).astype(bf16)

        cell, fcell = jt_ref[at, :], jc_ref[at, :]
        put(0, cell // 128)
        put(1, jk_ref[at, :] + 1)
        put(2, lax.rem(cell, 128))
        put(3, jnp.zeros_like(cell))
        put(4, (fcell // 128) * 16 + jf_ref[at, :])
        put(5, lax.rem(fcell, 128))
        return count + seen[:, 128:]

    lax.fori_loop(0, 32, chunk, jnp.zeros((128, 128), f32))
    slots = lax.dot_general(oht_ref[...], kv_ref[...], (((1,), (1,)), ((), ())), preferred_element_type=f32)
    first, second, third = slots[:, :128], slots[:, 128:256], slots[:, 256:]
    gain = jnp.zeros((128, 128), f32)
    for k in range(8):
        gain = jnp.where(first == float(k + 1), jcond_ref[k], gain)
    s0_ref[...] = jnp.where(lane < 64, first * 128.0 + second, gain)

    def turn(array):
        return pltpu.roll(array, 64, 1)

    def low_pair(array):
        return jnp.where(lane64 < 64, array[:64], turn(array[64:]))

    def high_pair(array):
        return jnp.where(lane64 < 64, turn(array[:64]), array[64:])

    row_ref[1] = low_pair(third).astype(i32)
    lane_ref[1] = high_pair(third).astype(i32)
    gain_ref[1] = high_pair(s0_ref[...])
    gain_ref[0] = jnp.ones((64, 128), f32)
    graw_ref[1] = gain_ref[1]

    pl.semaphore_wait(barrier, 127)

    own0 = pltpu.make_async_copy(s0_ref.at[pl.ds(me, 1)], r0_ref.at[pl.ds(me, 1)], r0sem)
    for ts, tp in peers:
        pltpu.make_async_remote_copy(
            src_ref=s0_ref.at[pl.ds(ts * 4 + tp, 1)], dst_ref=r0_ref.at[pl.ds(me, 1)],
            send_sem=s0sem, recv_sem=r0sem, device_id=(ts, tp), device_id_type=MESH,
        ).start()
    own0.start()

    def scatter(side, x):
        hi = x.astype(bf16)
        lo = (x - hi.astype(f32)).astype(bf16)
        total = jnp.zeros((128, 128), f32)
        for t in range(32):
            parts = []
            for i in (2 * t, 2 * t + 1):
                m = rmask_ref[side, i]
                parts.append(jnp.concatenate(
                    [m * jnp.broadcast_to(hi[i:i + 1], (64, 128)), m * jnp.broadcast_to(lo[i:i + 1], (64, 128))], axis=0))
            total = total + jnp.dot(
                jnp.concatenate(parts, axis=1), c_ref[side, t * 256:(t + 1) * 256, :], preferred_element_type=f32)
        return total[:64] + total[64:]

    def gather(side, v):
        hi = v.astype(bf16)
        lo = (v - hi.astype(f32)).astype(bf16)
        lhs = jnp.concatenate([hi, lo], axis=0)
        for t in range(32):
            p = jnp.dot(lhs, ct_ref[side, :, t * 256:(t + 1) * 256], preferred_element_type=f32)
            p = p[:64] + p[64:]
            for u in range(2):
                i = 2 * t + u
                read = jnp.sum(p[:, u * 128:(u + 1) * 128] * rmask_ref[side, i].astype(f32), axis=0, keepdims=True)
                s_ref[side, i:i + 1, :] = read * gain_ref[side, i:i + 1, :]

    def received(buffer):
        a, b = buffer[:64], buffer[64:]
        return jnp.where(lane64 < 64, pltpu.roll(a, 64 * half, 1), pltpu.roll(b, 64 * (1 - half), 1))

    def membrane(side, v):
        vh = 0.5 * v

        def pair(j, sums):
            conduct, driven = sums
            for u in range(2):
                k = 2 * j + u
                w = vh - prm_ref[0, k]
                factor = jnp.exp2(prm_ref[1, k] + prm_ref[2, k] * jnp.tanh(w))
                hc = prm_ref[3, k]
                swing = hc * jnp.tanh(w + w)
                steady = hc + swing if u == 0 else hc - swing
                old = y_ref[side, k].reshape(64, 128)
                new = steady + (old - steady) * factor
                y_ref[side, k] = new.reshape(4, 16, 128)
                conduct = conduct + new
                driven = driven + prm_ref[4, k] * new
            return conduct, driven

        zero = jnp.zeros((64, 128), f32)
        conduct, driven = lax.fori_loop(0, 20, pair, (zero, zero))
        return v * conduct - driven

    row16 = iota((16, 128), 0)
    lane16 = iota((16, 128), 1)

    def tissue_lap(par, slot):
        tiles = [v_ref[0, par, t] for t in range(4)]
        low = jnp.where(slab == 0, tiles[0], hb_ref[0, slot, 0])
        high = jnp.where(slab == 31, tiles[3], hb_ref[0, slot, 1])
        around = [low] + tiles + [high]
        out = []
        for t in range(4):
            here = tiles[t]
            ylo = jnp.where(plane == 0, here[0:1], hy_ref[slot, 0, t, 0:1, :])
            yhi = jnp.where(plane == 3, here[15:16], hy_ref[slot, 1, t, 0:1, :])
            total = around[t] + around[t + 2]
            total = total + jnp.where(row16 == 0, jnp.broadcast_to(ylo, (16, 128)), pltpu.roll(here, 1, 0))
            total = total + jnp.where(row16 == 15, jnp.broadcast_to(yhi, (16, 128)), pltpu.roll(here, 15, 0))
            total = total + jnp.where(lane16 == 0, here, pltpu.roll(here, 1, 1))
            total = total + jnp.where(lane16 == 127, here, pltpu.roll(here, 127, 1))
            out.append(total - 6.0 * here)
        return jnp.concatenate(out, axis=0)

    def fibre_lap(par, slot):
        tiles = [v_ref[1, par, t] for t in range(4)]
        around = [hb_ref[1, slot, 0]] + tiles + [hb_ref[1, slot, 1]]
        right = [pltpu.roll(a, 1, 1) for a in around[:5]]
        left = [pltpu.roll(a, 127, 1) for a in around[1:]]
        right[0] = jnp.where(plane == 0, tiles[0], right[0])
        left[4] = jnp.where(plane == 3, tiles[3], left[4])
        out = []
        for t in range(4):
            total = jnp.where(lane16 == 0, right[t], right[t + 1])
            total = total + jnp.where(lane16 == 127, left[t + 1], left[t])
            out.append(total - 2.0 * tiles[t])
        return jnp.concatenate(out, axis=0)

    def wait_rows(sem, rows):
        pltpu.make_async_copy(r0_ref.at[pl.ds(0, rows)], r0_ref.at[pl.ds(0, rows)], sem).wait()

    def wait_sends(side):
        wait_rows(ssem.at[side], 127)
        pltpu.make_async_copy(hb_ref.at[0, 0], hb_ref.at[0, 0], hssem.at[side]).wait()

        @pl.when(side == 0)
        def _():
            pltpu.make_async_copy(
                hy_ref.at[0, :, :, pl.ds(0, 1)], hy_ref.at[0, :, :, pl.ds(0, 1)], hssem.at[2]).wait()

    def act(m, carry):
        n = m // 2 - 1
        side = lax.rem(lax.rem(m, 2) + n + 2, 2)
        other = 1 - side
        par, slot = lax.rem(n + 2, 2), lax.rem(n + 4, 4)
        nxt, nslot = 1 - par, lax.rem(n + 5, 4)

        @pl.when(n >= 0)
        def _():
            v = v_ref[side, par].reshape(64, 128)
            ionic = membrane(side, v)
            pltpu.make_async_copy(hb_ref.at[0, 0], hb_ref.at[0, 0], hrsem.at[side, slot]).wait()

            def rest(lap):
                drift = d_ref[side].reshape(64, 128) * lap - ionic - gsum_ref[side] * v
                wait_rows(rsem.at[side, par], 127)
                x = received(r_ref[side, par]) * gain_ref[side]
                v_ref[side, nxt] = (v + DT * (drift + scatter(side, x))).reshape(4, 16, 128)

            @pl.when(side == 0)
            def _():
                pltpu.make_async_copy(
                    hy_ref.at[0, :, :, pl.ds(0, 1)], hy_ref.at[0, :, :, pl.ds(0, 1)], hrsem.at[2, slot]).wait()
                graw_ref[2] = tissue_lap(par, slot)

            @pl.when(side == 1)
            def _():
                graw_ref[2] = fibre_lap(par, slot)

            rest(graw_ref[2])

        @pl.when(n < 0)
        def _():
            @pl.when(side == 0)
            def _():
                wait_rows(r0sem, 128)
                table = r0_ref[...]
                cell = low_pair(table).astype(i32)
                row_ref[0] = cell // 128
                lane_ref[0] = lax.rem(cell, 128)
                graw_ref[0] = high_pair(table)

            def build(i, carry):
                at = pl.ds(i, 1)
                cols = pl.ds(pl.multiple_of(i * 128, 128), 128)
                rmask_ref[side, i] = jnp.where(
                    sub64 == jnp.broadcast_to(row_ref[side, at, :], (64, 128)), 1.0, 0.0).astype(bf16)
                ct_ref[side, :, cols] = jnp.where(
                    sub == jnp.broadcast_to(lane_ref[side, at, :], (128, 128)), 1.0, 0.0).astype(bf16)
                return carry

            lax.fori_loop(0, 64, build, 0)

        @pl.when(n < STEPS - 1)
        def _():
            @pl.when(n >= 0)
            def _():
                wait_sends(side)

            gather(side, v_ref[side, nxt].reshape(64, 128))
            r_ref[other, nxt, pl.ds(me, 1), :] = s_ref[side, pl.ds(q_me, 1), :]
            for ts, tp in peers:
                pltpu.make_async_remote_copy(
                    src_ref=s_ref.at[side, pl.ds(lax.rem(ts, 16) * 4 + tp, 1)],
                    dst_ref=r_ref.at[other, nxt, pl.ds(me, 1)],
                    send_sem=ssem.at[side], recv_sem=rsem.at[other, nxt],
                    device_id=(ts, tp), device_id_type=MESH,
                ).start()
            for up in (1, 0):
                ts = jnp.where(side == 0, lax.rem(slab + (1 if up else 31), 32), slab)
                tp = jnp.where(side == 0, plane, lax.rem(plane + (1 if up else 3), 4))
                pltpu.make_async_remote_copy(
                    src_ref=v_ref.at[side, nxt, 3 if up else 0], dst_ref=hb_ref.at[side, nslot, 1 - up],
                    send_sem=hssem.at[side], recv_sem=hrsem.at[side, nslot],
                    device_id=(ts, tp), device_id_type=MESH,
                ).start()

            @pl.when(side == 0)
            def _():
                for up in (1, 0):
                    pltpu.make_async_remote_copy(
                        src_ref=v_ref.at[0, nxt, :, pl.ds(15 if up else 0, 1)],
                        dst_ref=hy_ref.at[nslot, 1 - up, :, pl.ds(0, 1)],
                        send_sem=hssem.at[2], recv_sem=hrsem.at[2, nslot],
                        device_id=(slab, lax.rem(plane + (1 if up else 3), 4)), device_id_type=MESH,
                    ).start()

        @pl.when(n < 0)
        def _():
            def flip(i, carry):
                here = jnp.where(
                    sub == jnp.broadcast_to(lane_ref[side, pl.ds(i, 1), :], (128, 128)), 1.0, 0.0)
                c_ref[side, pl.ds(pl.multiple_of(i * 128, 128), 128), :] = here.T.astype(bf16)
                return carry

            lax.fori_loop(0, 64, flip, 0)
            gsum_ref[side] = scatter(side, graw_ref[side])

            @pl.when(side == 0)
            def _():
                loads[0].wait()

            @pl.when(side == 1)
            def _():
                for copy in loads[1:]:
                    copy.wait()

            def scale(k, carry):
                y_ref[side, k] = y_ref[side, k] * prm_ref[5, k]
                return carry

            lax.fori_loop(0, 40, scale, 0)

        return carry

    lax.fori_loop(0, 2 * STEPS + 2, act, 0)
    wait_rows(s0sem, 127)
    wait_sends(0)
    wait_sends(1)
    to_ref[...] = v_ref[0, STEPS % 2]
    for t in range(4):
        fo_ref[:, t * 128:(t + 1) * 128] = v_ref[1, STEPS % 2, t]


def body(
    tissue_v, tissue_gates, tissue_diff, fibre_v, fibre_gates, fibre_diff,
    gate_half, gate_rate, gate_cond, gate_rev, junc_cond,
    junc_fibre, junc_fcell, junc_owner, junc_tcell, junc_class,
):
    vmem, smem = pl.BlockSpec(memory_space=pltpu.VMEM), pl.BlockSpec(memory_space=pltpu.SMEM)
    anywhere = pl.BlockSpec(memory_space=pl.ANY)
    junctions = [a.reshape(32, 128) for a in (junc_fibre, junc_fcell, junc_owner[:, 0], junc_tcell, junc_class)]
    dma = pltpu.SemaphoreType.DMA
    return pl.pallas_call(
        kernel,
        out_shape=(jax.ShapeDtypeStruct((4, 16, 128), f32), jax.ShapeDtypeStruct((16, 512), f32)),
        in_specs=[vmem] * 4 + [anywhere] * 2 + [smem] * 5 + [vmem] * 5,
        out_specs=(vmem, vmem),
        scratch_shapes=[
            pltpu.VMEM((2, 2, 4, 16, 128), f32),
            pltpu.VMEM((2, 4, 16, 128), f32),
            pltpu.VMEM((2, 40, 4, 16, 128), f32),
            pltpu.SMEM((6, 40), f32),
            pltpu.VMEM((128, 4096), bf16),
            pltpu.VMEM((384, 4096), bf16),
            pltpu.VMEM((2, 64, 64, 128), bf16),
            pltpu.VMEM((2, 128, 8192), bf16),
            pltpu.VMEM((2, 8192, 128), bf16),
            pltpu.VMEM((2, 64, 128), i32),
            pltpu.VMEM((2, 64, 128), i32),
            pltpu.VMEM((2, 64, 128), f32),
            pltpu.VMEM((2, 64, 128), f32),
            pltpu.VMEM((3, 64, 128), f32),
            pltpu.VMEM((128, 128), f32),
            pltpu.VMEM((128, 128), f32),
            pltpu.VMEM((2, 64, 128), f32),
            pltpu.VMEM((2, 2, 128, 128), f32),
            pltpu.VMEM((2, 4, 2, 16, 128), f32),
            pltpu.VMEM((4, 2, 4, 8, 128), f32),
            dma((5,)), dma, dma, dma((2,)), dma((2, 2)), dma((3,)), dma((3, 4)),
        ],
        compiler_params=pltpu.CompilerParams(collective_id=0, has_side_effects=True),
    )(
        tissue_v, tissue_diff, fibre_v, fibre_diff, tissue_gates, fibre_gates,
        gate_half, gate_rate, gate_cond, gate_rev, junc_cond, *junctions,
    )


def solution(mesh):
    both = P(("slab", "plane"))
    in_specs = (
        P("slab", "plane", None), P(None, "slab", "plane", None), P("slab", "plane", None),
        P("slab", "plane"), P(None, "slab", "plane"), P("slab", "plane"),
        P(), P(), P(), P(), P(), both, both, P(("slab", "plane"), None), both, both,
    )
    out_specs = (P("slab", "plane", None), P("slab", "plane"))
    return jax.shard_map(body, mesh=mesh, in_specs=in_specs, out_specs=out_specs, check_vma=False)
```

```python
import jax
import jax.numpy as jnp
import numpy as np
from jax import lax
from jax.experimental import pallas as pl
from jax.experimental.pallas import tpu as pltpu
from jax.sharding import PartitionSpec as P

STEPS = 14
DT = 0.1
PARTS = 1
LOG2E = 1.4426950408889634
MESH = pl.DeviceIdType.MESH
f32, bf16, i32 = jnp.float32, jnp.bfloat16, jnp.int32


def rank_table():
    ring = lambda d: min(d, 4 - d)
    every = [(a, b, c, d) for a in range(4) for b in range(4) for c in range(2) for d in range(4)]
    far = lambda o: ring(o[0]) + ring(o[1]) + ring(o[3]) + 0.1 * o[2]
    streams, seen = ([], []), set()
    for o in sorted(every, key=lambda o: -far(o)):
        if o in seen:
            continue
        group = [o] if negative(o) == o else [o, negative(o)]
        seen.update(group)
        to = 0 if len(streams[0]) <= len(streams[1]) else 1
        if len(streams[to]) + len(group) > 64:
            to = 1 - to
        streams[to].extend(group)
    return streams[0] + streams[1]


def negative(o):
    return (-o[0] % 4, -o[1] % 4, o[2], -o[3] % 4)


RANKS = rank_table()
RANK_OF = {o: r for r, o in enumerate(RANKS)}
HERE = RANK_OF[(0, 0, 0, 0)]


def iota(shape, dim):
    return lax.broadcasted_iota(i32, shape, dim)


def kernel(
    tv_ref, td_ref, fv_ref, fd_ref, tg_ref, fg_ref,
    half_ref, rate_ref, cond_ref, rev_ref, jcond_ref,
    jf_ref, jc_ref, jo_ref, jt_ref, jk_ref, code_ref,
    to_ref, fo_ref,
    v_ref, d_ref, y_ref, prm_ref,
    oht_ref, kv_ref, rmask_ref, ct_ref, c_ref,
    row_ref, lane_ref, gain_ref, gsum_ref, graw_ref,
    s0_ref, r0_ref, s_ref, r_ref, hb_ref, hy_ref,
    gsem, s0sem, r0sem, ssem, rsem, hssem, hrsem,
):
    slab, plane = lax.axis_index("slab"), lax.axis_index("plane")
    z, y, core = slab // 8, lax.rem(slab // 2, 4), lax.rem(slab, 2)
    zs = [lax.rem(z + d, 4) * 8 for d in range(4)]
    ys = [lax.rem(y + d, 4) * 2 for d in range(4)]
    cs = [lax.rem(core + d, 2) for d in range(2)]
    xs = [lax.rem(plane + d, 4) for d in range(4)]

    def device(rank):
        a, b, c, d = RANKS[rank]
        return (zs[a] + ys[b] + cs[c], xs[d])

    peers = sorted((r for r in range(128) if r != HERE), key=lambda r: r % 64)

    loads = [pltpu.make_async_copy(tg_ref, y_ref.at[0], gsem.at[0])]
    for t in range(4):
        loads.append(pltpu.make_async_copy(fg_ref.at[:, :, pl.ds(t * 128, 128)], y_ref.at[1, :, t], gsem.at[1 + t]))
    for copy in loads:
        copy.start()

    barrier = pltpu.get_barrier_semaphore()

    for r in peers:
        pl.semaphore_signal(barrier, inc=1, device_id=device(r), device_id_type=MESH)

    def params(k, carry):
        rate, cond = rate_ref[k], cond_ref[k]
        prm_ref[6 * k + 0] = 0.5 * half_ref[k]
        prm_ref[6 * k + 1] = rate * (-1.5 * DT * LOG2E)
        prm_ref[6 * k + 2] = rate * (-0.5 * DT * LOG2E)
        prm_ref[6 * k + 3] = 0.5 * cond
        prm_ref[6 * k + 4] = rev_ref[k]
        prm_ref[6 * k + 5] = cond
        return carry

    lax.fori_loop(0, 40, params, 0)

    v_ref[0, 0] = tv_ref[...]
    d_ref[0] = td_ref[...]
    for t in range(4):
        v_ref[1, 0, t] = fv_ref[:, t * 128:(t + 1) * 128]
        d_ref[1, t] = fd_ref[:, t * 128:(t + 1) * 128]

    sub = iota((128, 128), 0)
    sub64 = iota((64, 128), 0)
    lane = iota((128, 128), 1)
    lane64 = iota((64, 128), 1)
    before = jnp.concatenate([jnp.where(sub < lane, 1.0, 0.0), jnp.ones((128, 128), f32)], axis=1).astype(bf16)

    def chunks(c4, count):
        for u in range(4):
            c = c4 * 4 + u
            at = pl.ds(c, 1)
            cols = pl.ds(pl.multiple_of(c * 128, 128), 128)
            owner = jo_ref[at, :]
            relative = (
                lax.rem(owner // 32 + 4 - z, 4) * 32 + lax.rem(lax.rem(owner // 8, 4) + 4 - y, 4) * 8
                + lax.rem(lax.rem(owner // 4, 2) + 2 - core, 2) * 4 + lax.rem(lax.rem(owner, 4) + 4 - plane, 4))
            hit = code_ref[...] == jnp.broadcast_to(relative, (128, 128))
            onehot = jnp.where(hit, 1.0, 0.0).astype(bf16)
            oht_ref[:, cols] = onehot
            seen = jnp.dot(onehot, before, preferred_element_type=f32)
            rank = jnp.sum(jnp.where(hit, seen[:, :128] + count, 0.0), axis=0, keepdims=True).astype(i32)
            place = sub64 == jnp.broadcast_to(rank, (64, 128))
            cell, fcell = jt_ref[at, :], jc_ref[at, :]
            planes = (
                cell // 128, jk_ref[at, :] + 1, lax.rem(cell, 128), jnp.zeros_like(cell),
                (fcell // 128) * 16 + jf_ref[at, :], lax.rem(fcell, 128))
            for p, value in enumerate(planes):
                value = jnp.broadcast_to(value.astype(f32), (64, 128))
                kv_ref[p * 64:(p + 1) * 64, cols] = jnp.where(place, value, 0.0).astype(bf16)
            count = count + seen[:, 128:]
        return count

    lax.fori_loop(0, 8, chunks, jnp.zeros((128, 128), f32))
    slots = lax.dot_general(oht_ref[...], kv_ref[...], (((1,), (1,)), ((), ())), preferred_element_type=f32)
    first, second, third = slots[:, :128], slots[:, 128:256], slots[:, 256:]
    gain = jnp.zeros((128, 128), f32)
    for k in range(8):
        gain = jnp.where(first == float(k + 1), jcond_ref[k], gain)
    s0_ref[...] = jnp.where(lane < 64, first * 128.0 + second, gain)

    def turn(array):
        return pltpu.roll(array, 64, 1)

    def low_pair(array):
        return jnp.where(lane64 < 64, array[:64], turn(array[64:]))

    def high_pair(array):
        return jnp.where(lane64 < 64, turn(array[:64]), array[64:])

    row_ref[1] = low_pair(third).astype(i32)
    lane_ref[1] = high_pair(third).astype(i32)
    gain_ref[1] = high_pair(s0_ref[...])
    gain_ref[0] = jnp.ones((64, 128), f32)
    graw_ref[1] = gain_ref[1]

    def send_tables():
        pl.semaphore_wait(barrier, 127)
        for r in peers:
            pltpu.make_async_remote_copy(
                src_ref=s0_ref.at[pl.ds(r, 1)], dst_ref=r0_ref.at[pl.ds(RANK_OF[negative(RANKS[r])], 1)],
                send_sem=s0sem, recv_sem=r0sem, device_id=device(r), device_id_type=MESH,
            ).start()
        r0_ref[HERE:HERE + 1, :] = s0_ref[HERE:HERE + 1, :]

    def send_row(side, nxt, i):
        for r in (i, i + 64):
            if r == HERE:
                r_ref[1 - side, nxt, HERE:HERE + 1, :] = s_ref[side, i:i + 1, :]
                continue
            to = RANK_OF[negative(RANKS[r])]
            pltpu.make_async_remote_copy(
                src_ref=s_ref.at[side, pl.ds(i, 1)], dst_ref=r_ref.at[1 - side, nxt, pl.ds(to, 1)],
                send_sem=ssem.at[side], recv_sem=rsem.at[1 - side, nxt, to % 64 // 32],
                device_id=device(r), device_id_type=MESH,
            ).start()

    def scatter(side, x, first):
        hi = x.astype(bf16)
        lo = (x - hi.astype(f32)).astype(bf16)
        total = jnp.zeros((128, 128), f32)
        for t in range(x.shape[0] // 2):
            parts = []
            for i in (2 * t, 2 * t + 1):
                m = rmask_ref[side, 2 * first + i]
                parts.append(jnp.concatenate(
                    [m * jnp.broadcast_to(hi[i:i + 1], (64, 128)), m * jnp.broadcast_to(lo[i:i + 1], (64, 128))], axis=0))
            at = (first + t) * 256
            total = total + jnp.dot(
                jnp.concatenate(parts, axis=1), c_ref[side, at:at + 256, :], preferred_element_type=f32)
        return total[:64] + total[64:]

    def gather(side, v, nxt, send):
        hi = v.astype(bf16)
        lo = (v - hi.astype(f32)).astype(bf16)
        lhs = jnp.concatenate([hi, lo], axis=0)
        for part in range(PARTS):
            rows = 64 // PARTS
            for t in range(part * rows // 2, (part + 1) * rows // 2):
                p = jnp.dot(lhs, ct_ref[side, :, t * 256:(t + 1) * 256], preferred_element_type=f32)
                p = p[:64] + p[64:]
                for u in range(2):
                    i = 2 * t + u
                    read = jnp.sum(p[:, u * 128:(u + 1) * 128] * rmask_ref[side, i].astype(f32), axis=0, keepdims=True)
                    s_ref[side, i:i + 1, :] = read * gain_ref[side, i:i + 1, :]
            for i in range(part * rows, (part + 1) * rows):
                send(side, nxt, i)

    def received(side, par, low):
        a = r_ref[side, par, low:low + 32, :]
        b = r_ref[side, par, 64 + low:96 + low, :]
        return jnp.where(lane64[:32] < 64, a, b) * gain_ref[side, low:low + 32, :]

    def membrane(side, par):
        out = []
        for h in range(2):
            v = v_ref[side, par, 2 * h:2 * h + 2].reshape(32, 128)
            vh = 0.5 * v

            def some(j, sums):
                conduct, driven = sums
                for u in range(8):
                    k = 8 * j + u
                    w = vh - prm_ref[6 * k]
                    factor = jnp.exp2(prm_ref[6 * k + 1] + prm_ref[6 * k + 2] * jnp.tanh(w))
                    hc = prm_ref[6 * k + 3]
                    swing = hc * jnp.tanh(w + w)
                    steady = hc + swing if u % 2 == 0 else hc - swing
                    old = y_ref[side, k, 2 * h:2 * h + 2].reshape(32, 128)
                    new = steady + (old - steady) * factor
                    y_ref[side, k, 2 * h:2 * h + 2] = new.reshape(2, 16, 128)
                    conduct = conduct + new
                    driven = driven + prm_ref[6 * k + 4] * new
                return conduct, driven

            zero = jnp.zeros((32, 128), f32)
            conduct, driven = lax.fori_loop(0, 5, some, (zero, zero))
            out.append(v * conduct - driven)
        return jnp.concatenate(out, axis=0)

    row16 = iota((16, 128), 0)
    lane16 = iota((16, 128), 1)

    def tissue_inner(par):
        tiles = [v_ref[0, par, t] for t in range(4)]
        around = [jnp.zeros((16, 128), f32)] + tiles + [jnp.zeros((16, 128), f32)]
        out = []
        for t in range(4):
            here = tiles[t]
            total = around[t] + around[t + 2]
            total = total + jnp.where(row16 == 0, 0.0, pltpu.roll(here, 1, 0))
            total = total + jnp.where(row16 == 15, 0.0, pltpu.roll(here, 15, 0))
            total = total + jnp.where(lane16 == 0, here, pltpu.roll(here, 1, 1))
            total = total + jnp.where(lane16 == 127, here, pltpu.roll(here, 127, 1))
            out.append(total - 6.0 * here)
        return jnp.concatenate(out, axis=0)

    def tissue_outer(par, slot):
        tiles = [v_ref[0, par, t] for t in range(4)]
        out = []
        for t in range(4):
            here = tiles[t]
            ylo = jnp.where(plane == 0, here[0:1], hy_ref[slot, 0, t, 0:1, :])
            yhi = jnp.where(plane == 3, here[15:16], hy_ref[slot, 1, t, 0:1, :])
            out.append(jnp.where(row16 == 0, jnp.broadcast_to(ylo, (16, 128)), 0.0)
                       + jnp.where(row16 == 15, jnp.broadcast_to(yhi, (16, 128)), 0.0))
        out[0] = out[0] + jnp.where(slab == 0, tiles[0], hb_ref[0, slot, 0])
        out[3] = out[3] + jnp.where(slab == 31, tiles[3], hb_ref[0, slot, 1])
        return jnp.concatenate(out, axis=0)

    def fibre_inner(par):
        tiles = [v_ref[1, par, t] for t in range(4)]
        right = [jnp.zeros((16, 128), f32)] + [pltpu.roll(a, 1, 1) for a in tiles]
        left = [pltpu.roll(a, 127, 1) for a in tiles] + [jnp.zeros((16, 128), f32)]
        out = []
        for t in range(4):
            total = jnp.where(lane16 == 0, right[t], right[t + 1])
            total = total + jnp.where(lane16 == 127, left[t + 1], left[t])
            out.append(total - 2.0 * tiles[t])
        return jnp.concatenate(out, axis=0)

    def fibre_outer(par, slot):
        right = jnp.where(plane == 0, v_ref[1, par, 0], pltpu.roll(hb_ref[1, slot, 0], 1, 1))
        left = jnp.where(plane == 3, v_ref[1, par, 3], pltpu.roll(hb_ref[1, slot, 1], 127, 1))
        none = jnp.zeros((16, 128), f32)
        return jnp.concatenate(
            [jnp.where(lane16 == 0, right, 0.0), none, none, jnp.where(lane16 == 127, left, 0.0)], axis=0)

    def wait_rows(sem, rows):
        pltpu.make_async_copy(r0_ref.at[pl.ds(0, rows)], r0_ref.at[pl.ds(0, rows)], sem).wait()

    def wait_tiles(sem):
        pltpu.make_async_copy(hb_ref.at[0, 0], hb_ref.at[0, 0], sem).wait()

    def wait_lines(sem):
        pltpu.make_async_copy(hy_ref.at[0, :, :, pl.ds(0, 1)], hy_ref.at[0, :, :, pl.ds(0, 1)], sem).wait()

    def wait_edges_sent(side):
        wait_tiles(hssem.at[side])

        @pl.when(side == 0)
        def _():
            wait_lines(hssem.at[2])

    def prepare(side):
        def flip(i8, carry):
            for u in range(8):
                i = i8 * 8 + u
                here = jnp.where(
                    sub == jnp.broadcast_to(lane_ref[side, pl.ds(i, 1), :], (128, 128)), 1.0, 0.0)
                c_ref[side, pl.ds(pl.multiple_of(i * 128, 128), 128), :] = here.T.astype(bf16)
            return carry

        lax.fori_loop(0, 8, flip, 0)
        gsum_ref[side] = scatter(side, graw_ref[side], 0)
        for copy in loads[:1] if side == 0 else loads[1:]:
            copy.wait()

        def scale(k, carry):
            y_ref[side, k] = y_ref[side, k] * prm_ref[6 * k + 5]
            return carry

        lax.fori_loop(0, 40, scale, 0)

    def act(m, carry):
        n = m // 2 - 1
        side = lax.rem(lax.rem(m, 2) + n + 2, 2)
        other = 1 - side
        par, slot = lax.rem(n + 2, 2), lax.rem(n + 4, 4)
        nxt, nslot = 1 - par, lax.rem(n + 5, 4)

        @pl.when(n >= 0)
        def _():
            v = v_ref[side, par].reshape(64, 128)
            graw_ref[2] = v - DT * (membrane(side, par) + gsum_ref[side] * v)
            diffusion = d_ref[side].reshape(64, 128)

            @pl.when(side == 0)
            def _():
                graw_ref[2] = graw_ref[2] + DT * diffusion * tissue_inner(par)

            @pl.when(side == 1)
            def _():
                graw_ref[2] = graw_ref[2] + DT * diffusion * fibre_inner(par)

            wait_rows(rsem.at[side, par, 1], 63)
            source = scatter(side, received(side, par, 32), 16)
            wait_rows(rsem.at[side, par, 0], 64)
            source = source + scatter(side, received(side, par, 0), 0)
            known = graw_ref[2] + DT * source
            wait_tiles(hrsem.at[side, slot])

            @pl.when(side == 0)
            def _():
                wait_lines(hrsem.at[2, slot])
                v_ref[0, nxt] = (known + DT * diffusion * tissue_outer(par, slot)).reshape(4, 16, 128)

            @pl.when(side == 1)
            def _():
                v_ref[1, nxt] = (known + DT * diffusion * fibre_outer(par, slot)).reshape(4, 16, 128)

        @pl.when(n < 0)
        def _():
            @pl.when(side == 0)
            def _():
                wait_rows(r0sem, 127)
                table = r0_ref[...]
                cell = low_pair(table).astype(i32)
                row_ref[0] = cell // 128
                lane_ref[0] = lax.rem(cell, 128)
                graw_ref[0] = high_pair(table)

            def build(i4, carry):
                for u in range(4):
                    i = i4 * 4 + u
                    at = pl.ds(i, 1)
                    cols = pl.ds(pl.multiple_of(i * 128, 128), 128)
                    rmask_ref[side, i] = jnp.where(
                        sub64 == jnp.broadcast_to(row_ref[side, at, :], (64, 128)), 1.0, 0.0).astype(bf16)
                    ct_ref[side, :, cols] = jnp.where(
                        sub == jnp.broadcast_to(lane_ref[side, at, :], (128, 128)), 1.0, 0.0).astype(bf16)
                return carry

            lax.fori_loop(0, 16, build, 0)

        @pl.when(m == 0)
        def _():
            prepare(1)
            send_tables()

        @pl.when(n < STEPS - 1)
        def _():
            @pl.when(n >= 0)
            def _():
                wait_edges_sent(side)
                wait_rows(ssem.at[side], 127)

            for up in (1, 0):
                ts = jnp.where(side == 0, lax.rem(slab + (1 if up else 31), 32), slab)
                tp = jnp.where(side == 0, plane, lax.rem(plane + (1 if up else 3), 4))
                pltpu.make_async_remote_copy(
                    src_ref=v_ref.at[side, nxt, 3 if up else 0], dst_ref=hb_ref.at[side, nslot, 1 - up],
                    send_sem=hssem.at[side], recv_sem=hrsem.at[side, nslot],
                    device_id=(ts, tp), device_id_type=MESH,
                ).start()

            @pl.when(side == 0)
            def _():
                for up in (1, 0):
                    pltpu.make_async_remote_copy(
                        src_ref=v_ref.at[0, nxt, :, pl.ds(15 if up else 0, 1)],
                        dst_ref=hy_ref.at[nslot, 1 - up, :, pl.ds(0, 1)],
                        send_sem=hssem.at[2], recv_sem=hrsem.at[2, nslot],
                        device_id=(slab, lax.rem(plane + (1 if up else 3), 4)), device_id_type=MESH,
                    ).start()

            gather(side, v_ref[side, nxt].reshape(64, 128), nxt, send_row)

        @pl.when(m == 1)
        def _():
            prepare(0)

        return carry

    lax.fori_loop(0, 2 * STEPS + 2, act, 0)
    wait_rows(s0sem, 127)
    for side in range(2):
        wait_rows(ssem.at[side], 127)
        wait_tiles(hssem.at[side])
    wait_lines(hssem.at[2])
    to_ref[...] = v_ref[0, STEPS % 2]
    for t in range(4):
        fo_ref[:, t * 128:(t + 1) * 128] = v_ref[1, STEPS % 2, t]


def body(
    tissue_v, tissue_gates, tissue_diff, fibre_v, fibre_gates, fibre_diff,
    gate_half, gate_rate, gate_cond, gate_rev, junc_cond,
    junc_fibre, junc_fcell, junc_owner, junc_tcell, junc_class,
):
    vmem, smem = pl.BlockSpec(memory_space=pltpu.VMEM), pl.BlockSpec(memory_space=pltpu.SMEM)
    anywhere = pl.BlockSpec(memory_space=pl.ANY)
    junctions = [a.reshape(32, 128) for a in (junc_fibre, junc_fcell, junc_owner[:, 0], junc_tcell, junc_class)]
    dma = pltpu.SemaphoreType.DMA
    codes = np.array([[a * 32 + b * 8 + c * 4 + d] * 128 for a, b, c, d in RANKS], np.int32)
    return pl.pallas_call(
        kernel,
        out_shape=(jax.ShapeDtypeStruct((4, 16, 128), f32), jax.ShapeDtypeStruct((16, 512), f32)),
        in_specs=[vmem] * 4 + [anywhere] * 2 + [smem] * 5 + [vmem] * 6,
        out_specs=(vmem, vmem),
        scratch_shapes=[
            pltpu.VMEM((2, 2, 4, 16, 128), f32),
            pltpu.VMEM((2, 4, 16, 128), f32),
            pltpu.VMEM((2, 40, 4, 16, 128), f32),
            pltpu.SMEM((240,), f32),
            pltpu.VMEM((128, 4096), bf16),
            pltpu.VMEM((384, 4096), bf16),
            pltpu.VMEM((2, 64, 64, 128), bf16),
            pltpu.VMEM((2, 128, 8192), bf16),
            pltpu.VMEM((2, 8192, 128), bf16),
            pltpu.VMEM((2, 64, 128), i32),
            pltpu.VMEM((2, 64, 128), i32),
            pltpu.VMEM((2, 64, 128), f32),
            pltpu.VMEM((2, 64, 128), f32),
            pltpu.VMEM((3, 64, 128), f32),
            pltpu.VMEM((128, 128), f32),
            pltpu.VMEM((128, 128), f32),
            pltpu.VMEM((2, 64, 128), f32),
            pltpu.VMEM((2, 2, 128, 128), f32),
            pltpu.VMEM((2, 4, 2, 16, 128), f32),
            pltpu.VMEM((4, 2, 4, 8, 128), f32),
            dma((5,)), dma, dma, dma((2,)), dma((2, 2, 2)), dma((3,)), dma((3, 4)),
        ],
        compiler_params=pltpu.CompilerParams(collective_id=0, has_side_effects=True),
    )(
        tissue_v, tissue_diff, fibre_v, fibre_diff, tissue_gates, fibre_gates,
        gate_half, gate_rate, gate_cond, gate_rev, junc_cond, *junctions, codes,
    )


def solution(mesh):
    both = P(("slab", "plane"))
    in_specs = (
        P("slab", "plane", None), P(None, "slab", "plane", None), P("slab", "plane", None),
        P("slab", "plane"), P(None, "slab", "plane"), P("slab", "plane"),
        P(), P(), P(), P(), P(), both, both, P(("slab", "plane"), None), both, both,
    )
    out_specs = (P("slab", "plane", None), P("slab", "plane"))
    return jax.shard_map(body, mesh=mesh, in_specs=in_specs, out_specs=out_specs, check_vma=False)
```

```python
import jax
import jax.numpy as jnp
import numpy as np
from jax import lax
from jax.experimental import pallas as pl
from jax.experimental.pallas import tpu as pltpu
from jax.sharding import PartitionSpec as P

STEPS = 14
DT = 0.1
CUTS = (0, 64)
GROUPS = (0,)
LOG2E = 1.4426950408889634
MESH = pl.DeviceIdType.MESH
f32, bf16, i32 = jnp.float32, jnp.bfloat16, jnp.int32


def rank_table():
    ring = lambda d: min(d, 4 - d)
    every = [(a, b, c, d) for a in range(4) for b in range(4) for c in range(2) for d in range(4)]
    far = lambda o: ring(o[0]) + ring(o[1]) + ring(o[3]) + 0.1 * o[2]
    streams, seen = ([], []), set()
    for o in sorted(every, key=lambda o: -far(o)):
        if o in seen:
            continue
        group = [o] if negative(o) == o else [o, negative(o)]
        seen.update(group)
        to = 0 if len(streams[0]) <= len(streams[1]) else 1
        if len(streams[to]) + len(group) > 64:
            to = 1 - to
        streams[to].extend(group)
    return streams[0] + streams[1]


def negative(o):
    return (-o[0] % 4, -o[1] % 4, o[2], -o[3] % 4)


RANKS = rank_table()
RANK_OF = {o: r for r, o in enumerate(RANKS)}
HERE = RANK_OF[(0, 0, 0, 0)]


def iota(shape, dim):
    return lax.broadcasted_iota(i32, shape, dim)


def kernel(
    tv_ref, td_ref, fv_ref, fd_ref, tg_ref, fg_ref,
    half_in, rate_in, cond_in, rev_in, jcond_in,
    jf_in, jc_in, jo_in, jt_in, jk_in, code_in,
    out_ref,
    half_ref, rate_ref, cond_ref, rev_ref, jcond_ref,
    jf_ref, jc_ref, jo_ref, jt_ref, jk_ref, code_ref,
    v_ref, d_ref, y_ref, prm_ref,
    oht_ref, kv_ref, rmask_ref, ct_ref, c_ref,
    row_ref, lane_ref, gain_ref, gsum_ref, graw_ref,
    s0_ref, r0_ref, s_ref, r_ref, hb_ref, hy_ref,
    gsem, s0sem, r0sem, ssem, rsem, hssem, hrsem, isem,
):
    slab, plane = lax.axis_index("slab"), lax.axis_index("plane")
    z, y, core = slab // 8, lax.rem(slab // 2, 4), lax.rem(slab, 2)
    zs = [lax.rem(z + d, 4) * 8 for d in range(4)]
    ys = [lax.rem(y + d, 4) * 2 for d in range(4)]
    cs = [lax.rem(core + d, 2) for d in range(2)]
    xs = [lax.rem(plane + d, 4) for d in range(4)]

    def device(rank):
        a, b, c, d = RANKS[rank]
        return (zs[a] + ys[b] + cs[c], xs[d])

    peers = sorted((r for r in range(128) if r != HERE), key=lambda r: r % 64)

    barrier = pltpu.get_barrier_semaphore()
    for r in peers:
        pl.semaphore_signal(barrier, inc=1, device_id=device(r), device_id_type=MESH)

    pairs = [
        (jo_in, jo_ref), (code_in, code_ref), (jt_in, jt_ref), (jk_in, jk_ref), (jc_in, jc_ref), (jf_in, jf_ref),
        (jcond_in, jcond_ref), (half_in, half_ref), (rate_in, rate_ref), (cond_in, cond_ref), (rev_in, rev_ref),
        (tv_ref, v_ref.at[0, 0]), (td_ref, d_ref.at[0])]
    for t in range(4):
        pairs.append((fv_ref.at[:, pl.ds(t * 128, 128)], v_ref.at[1, 0, t]))
        pairs.append((fd_ref.at[:, pl.ds(t * 128, 128)], d_ref.at[1, t]))
    arrivals = [pltpu.make_async_copy(a, b, isem.at[k]) for k, (a, b) in enumerate(pairs)]
    loads = [pltpu.make_async_copy(tg_ref, y_ref.at[0], gsem.at[0])]
    for t in range(4):
        loads.append(pltpu.make_async_copy(fg_ref.at[:, :, pl.ds(t * 128, 128)], y_ref.at[1, :, t], gsem.at[1 + t]))
    for copy in arrivals + loads:
        copy.start()
    for copy in arrivals:
        copy.wait()

    def params(k, carry):
        rate, cond = rate_ref[k], cond_ref[k]
        prm_ref[6 * k + 0] = 0.5 * half_ref[k]
        prm_ref[6 * k + 1] = rate * (-1.5 * DT * LOG2E)
        prm_ref[6 * k + 2] = rate * (-0.5 * DT * LOG2E)
        prm_ref[6 * k + 3] = 0.5 * cond
        prm_ref[6 * k + 4] = rev_ref[k]
        prm_ref[6 * k + 5] = cond
        return carry

    lax.fori_loop(0, 40, params, 0)

    sub = iota((128, 128), 0)
    sub64 = iota((64, 128), 0)
    lane = iota((128, 128), 1)
    lane64 = iota((64, 128), 1)
    before = jnp.concatenate([jnp.where(sub < lane, 1.0, 0.0), jnp.ones((128, 128), f32)], axis=1).astype(bf16)

    def chunks(c4, count):
        for u in range(4):
            c = c4 * 4 + u
            at = pl.ds(c, 1)
            cols = pl.ds(pl.multiple_of(c * 128, 128), 128)
            owner = jo_ref[at, :]
            relative = (
                lax.rem(owner // 32 + 4 - z, 4) * 32 + lax.rem(lax.rem(owner // 8, 4) + 4 - y, 4) * 8
                + lax.rem(lax.rem(owner // 4, 2) + 2 - core, 2) * 4 + lax.rem(lax.rem(owner, 4) + 4 - plane, 4))
            hit = code_ref[...] == jnp.broadcast_to(relative, (128, 128))
            onehot = jnp.where(hit, 1.0, 0.0).astype(bf16)
            oht_ref[:, cols] = onehot
            seen = jnp.dot(onehot, before, preferred_element_type=f32)
            rank = jnp.sum(jnp.where(hit, seen[:, :128] + count, 0.0), axis=0, keepdims=True).astype(i32)
            place = sub64 == jnp.broadcast_to(rank, (64, 128))
            cell, fcell = jt_ref[at, :], jc_ref[at, :]
            planes = (
                cell // 128, jk_ref[at, :] + 1, lax.rem(cell, 128), jnp.zeros_like(cell),
                (fcell // 128) * 16 + jf_ref[at, :], lax.rem(fcell, 128))
            for p, value in enumerate(planes):
                value = jnp.broadcast_to(value.astype(f32), (64, 128))
                kv_ref[p * 64:(p + 1) * 64, cols] = jnp.where(place, value, 0.0).astype(bf16)
            count = count + seen[:, 128:]
        return count

    lax.fori_loop(0, 8, chunks, jnp.zeros((128, 128), f32))
    slots = lax.dot_general(oht_ref[...], kv_ref[...], (((1,), (1,)), ((), ())), preferred_element_type=f32)
    first, second, third = slots[:, :128], slots[:, 128:256], slots[:, 256:]
    gain = jnp.zeros((128, 128), f32)
    for k in range(8):
        gain = jnp.where(first == float(k + 1), jcond_ref[k], gain)
    s0_ref[...] = jnp.where(lane < 64, first * 128.0 + second, gain)

    def turn(array):
        return pltpu.roll(array, 64, 1)

    def low_pair(array):
        return jnp.where(lane64 < 64, array[:64], turn(array[64:]))

    def high_pair(array):
        return jnp.where(lane64 < 64, turn(array[:64]), array[64:])

    row_ref[1] = low_pair(third).astype(i32)
    lane_ref[1] = high_pair(third).astype(i32)
    gain_ref[1] = high_pair(s0_ref[...])
    gain_ref[0] = jnp.ones((64, 128), f32)
    graw_ref[1] = gain_ref[1]

    def send_tables():
        pl.semaphore_wait(barrier, 127)
        for r in peers:
            pltpu.make_async_remote_copy(
                src_ref=s0_ref.at[pl.ds(r, 1)], dst_ref=r0_ref.at[pl.ds(RANK_OF[negative(RANKS[r])], 1)],
                send_sem=s0sem, recv_sem=r0sem, device_id=device(r), device_id_type=MESH,
            ).start()
        r0_ref[HERE:HERE + 1, :] = s0_ref[HERE:HERE + 1, :]

    def send_row(side, nxt, i):
        for r in (i, i + 64):
            if r == HERE:
                r_ref[1 - side, nxt, HERE:HERE + 1, :] = s_ref[side, i:i + 1, :]
                continue
            to = RANK_OF[negative(RANKS[r])]
            pltpu.make_async_remote_copy(
                src_ref=s_ref.at[side, pl.ds(i, 1)], dst_ref=r_ref.at[1 - side, nxt, pl.ds(to, 1)],
                send_sem=ssem.at[side], recv_sem=rsem.at[1 - side, nxt, sum(to % 64 < g for g in GROUPS)],
                device_id=device(r), device_id_type=MESH,
            ).start()

    def scatter(side, x, first, total):
        hi = x.astype(bf16)
        lo = (x - hi.astype(f32)).astype(bf16)
        for t in range(0, x.shape[0], 2):
            parts = []
            for i in (t, t + 1):
                m = rmask_ref[side, first + i]
                parts.append(jnp.concatenate(
                    [m * jnp.broadcast_to(hi[i:i + 1], (64, 128)), m * jnp.broadcast_to(lo[i:i + 1], (64, 128))], axis=0))
            at = (first + t) * 128
            total = total + jnp.dot(
                jnp.concatenate(parts, axis=1), c_ref[side, at:at + 256, :], preferred_element_type=f32)
        return total

    def gather(side, v, nxt, send):
        hi = v.astype(bf16)
        lo = (v - hi.astype(f32)).astype(bf16)
        lhs = jnp.concatenate([hi, lo], axis=0)
        for start, stop in zip(CUTS, CUTS[1:]):
            for t in range(start // 2, stop // 2):
                p = jnp.dot(lhs, ct_ref[side, :, t * 256:(t + 1) * 256], preferred_element_type=f32)
                p = p[:64] + p[64:]
                for u in range(2):
                    i = 2 * t + u
                    read = jnp.sum(p[:, u * 128:(u + 1) * 128] * rmask_ref[side, i].astype(f32), axis=0, keepdims=True)
                    s_ref[side, i:i + 1, :] = read * gain_ref[side, i:i + 1, :]
            for i in range(start, stop):
                send(side, nxt, i)

    def received(side, par, low, high):
        a = r_ref[side, par, low:high, :]
        b = r_ref[side, par, 64 + low:64 + high, :]
        return jnp.where(lane64[:high - low] < 64, a, b) * gain_ref[side, low:high, :]

    def membrane(side, par):
        out = []
        for h in range(2):
            v = v_ref[side, par, 2 * h:2 * h + 2].reshape(32, 128)
            vh = 0.5 * v

            def some(j, sums):
                conduct, driven = sums
                for u in range(8):
                    k = 8 * j + u
                    w = vh - prm_ref[6 * k]
                    factor = jnp.exp2(prm_ref[6 * k + 1] + prm_ref[6 * k + 2] * jnp.tanh(w))
                    hc = prm_ref[6 * k + 3]
                    swing = hc * jnp.tanh(w + w)
                    steady = hc + swing if u % 2 == 0 else hc - swing
                    old = y_ref[side, k, 2 * h:2 * h + 2].reshape(32, 128)
                    new = steady + (old - steady) * factor
                    y_ref[side, k, 2 * h:2 * h + 2] = new.reshape(2, 16, 128)
                    conduct = conduct + new
                    driven = driven + prm_ref[6 * k + 4] * new
                return conduct, driven

            zero = jnp.zeros((32, 128), f32)
            conduct, driven = lax.fori_loop(0, 5, some, (zero, zero))
            out.append(v * conduct - driven)
        return jnp.concatenate(out, axis=0)

    row16 = iota((16, 128), 0)
    lane16 = iota((16, 128), 1)

    def tissue_inner(par):
        tiles = [v_ref[0, par, t] for t in range(4)]
        around = [jnp.zeros((16, 128), f32)] + tiles + [jnp.zeros((16, 128), f32)]
        out = []
        for t in range(4):
            here = tiles[t]
            total = around[t] + around[t + 2]
            total = total + jnp.where(row16 == 0, 0.0, pltpu.roll(here, 1, 0))
            total = total + jnp.where(row16 == 15, 0.0, pltpu.roll(here, 15, 0))
            total = total + jnp.where(lane16 == 0, here, pltpu.roll(here, 1, 1))
            total = total + jnp.where(lane16 == 127, here, pltpu.roll(here, 127, 1))
            out.append(total - 6.0 * here)
        return jnp.concatenate(out, axis=0)

    def tissue_outer(par, slot):
        tiles = [v_ref[0, par, t] for t in range(4)]
        out = []
        for t in range(4):
            here = tiles[t]
            ylo = jnp.where(plane == 0, here[0:1], hy_ref[slot, 0, t, 0:1, :])
            yhi = jnp.where(plane == 3, here[15:16], hy_ref[slot, 1, t, 0:1, :])
            out.append(jnp.where(row16 == 0, jnp.broadcast_to(ylo, (16, 128)), 0.0)
                       + jnp.where(row16 == 15, jnp.broadcast_to(yhi, (16, 128)), 0.0))
        out[0] = out[0] + jnp.where(slab == 0, tiles[0], hb_ref[0, slot, 0])
        out[3] = out[3] + jnp.where(slab == 31, tiles[3], hb_ref[0, slot, 1])
        return jnp.concatenate(out, axis=0)

    def fibre_inner(par):
        tiles = [v_ref[1, par, t] for t in range(4)]
        right = [jnp.zeros((16, 128), f32)] + [pltpu.roll(a, 1, 1) for a in tiles]
        left = [pltpu.roll(a, 127, 1) for a in tiles] + [jnp.zeros((16, 128), f32)]
        out = []
        for t in range(4):
            total = jnp.where(lane16 == 0, right[t], right[t + 1])
            total = total + jnp.where(lane16 == 127, left[t + 1], left[t])
            out.append(total - 2.0 * tiles[t])
        return jnp.concatenate(out, axis=0)

    def fibre_outer(par, slot):
        right = jnp.where(plane == 0, v_ref[1, par, 0], pltpu.roll(hb_ref[1, slot, 0], 1, 1))
        left = jnp.where(plane == 3, v_ref[1, par, 3], pltpu.roll(hb_ref[1, slot, 1], 127, 1))
        none = jnp.zeros((16, 128), f32)
        return jnp.concatenate(
            [jnp.where(lane16 == 0, right, 0.0), none, none, jnp.where(lane16 == 127, left, 0.0)], axis=0)

    def wait_rows(sem, rows):
        pltpu.make_async_copy(r0_ref.at[pl.ds(0, rows)], r0_ref.at[pl.ds(0, rows)], sem).wait()

    def wait_tiles(sem):
        pltpu.make_async_copy(hb_ref.at[0, 0], hb_ref.at[0, 0], sem).wait()

    def wait_lines(sem):
        pltpu.make_async_copy(hy_ref.at[0, :, :, pl.ds(0, 1)], hy_ref.at[0, :, :, pl.ds(0, 1)], sem).wait()

    def wait_edges_sent(side):
        wait_tiles(hssem.at[side])

        @pl.when(side == 0)
        def _():
            wait_lines(hssem.at[2])

    def prepare(side):
        def flip(i8, carry):
            for u in range(8):
                i = i8 * 8 + u
                here = jnp.where(
                    sub == jnp.broadcast_to(lane_ref[side, pl.ds(i, 1), :], (128, 128)), 1.0, 0.0)
                c_ref[side, pl.ds(pl.multiple_of(i * 128, 128), 128), :] = here.T.astype(bf16)
            return carry

        lax.fori_loop(0, 8, flip, 0)
        total = scatter(side, graw_ref[side], 0, jnp.zeros((128, 128), f32))
        gsum_ref[side] = total[:64] + total[64:]
        for copy in loads[:1] if side == 0 else loads[1:]:
            copy.wait()

        def scale(k, carry):
            y_ref[side, k] = y_ref[side, k] * prm_ref[6 * k + 5]
            return carry

        lax.fori_loop(0, 40, scale, 0)

    def act(m, carry):
        n = m // 2 - 1
        side = lax.rem(lax.rem(m, 2) + n + 2, 2)
        other = 1 - side
        par, slot = lax.rem(n + 2, 2), lax.rem(n + 4, 4)
        nxt, nslot = 1 - par, lax.rem(n + 5, 4)

        @pl.when(n >= 0)
        def _():
            v = v_ref[side, par].reshape(64, 128)
            graw_ref[2] = v - DT * (membrane(side, par) + gsum_ref[side] * v)
            diffusion = d_ref[side].reshape(64, 128)

            @pl.when(side == 0)
            def _():
                graw_ref[2] = graw_ref[2] + DT * diffusion * tissue_inner(par)

            @pl.when(side == 1)
            def _():
                graw_ref[2] = graw_ref[2] + DT * diffusion * fibre_inner(par)

            total, high = jnp.zeros((128, 128), f32), 64
            for g, low in enumerate(GROUPS):
                wait_rows(rsem.at[side, par, g], 2 * (high - low) - (low <= HERE % 64 < high))
                total = scatter(side, received(side, par, low, high), low, total)
                high = low
            known = graw_ref[2] + DT * (total[:64] + total[64:])
            wait_tiles(hrsem.at[side, slot])

            @pl.when(side == 0)
            def _():
                wait_lines(hrsem.at[2, slot])
                v_ref[0, nxt] = (known + DT * diffusion * tissue_outer(par, slot)).reshape(4, 16, 128)

            @pl.when(side == 1)
            def _():
                v_ref[1, nxt] = (known + DT * diffusion * fibre_outer(par, slot)).reshape(4, 16, 128)

        @pl.when(n < 0)
        def _():
            @pl.when(side == 0)
            def _():
                wait_rows(r0sem, 127)
                table = r0_ref[...]
                cell = low_pair(table).astype(i32)
                row_ref[0] = cell // 128
                lane_ref[0] = lax.rem(cell, 128)
                graw_ref[0] = high_pair(table)

            def build(i4, carry):
                for u in range(4):
                    i = i4 * 4 + u
                    at = pl.ds(i, 1)
                    cols = pl.ds(pl.multiple_of(i * 128, 128), 128)
                    rmask_ref[side, i] = jnp.where(
                        sub64 == jnp.broadcast_to(row_ref[side, at, :], (64, 128)), 1.0, 0.0).astype(bf16)
                    ct_ref[side, :, cols] = jnp.where(
                        sub == jnp.broadcast_to(lane_ref[side, at, :], (128, 128)), 1.0, 0.0).astype(bf16)
                return carry

            lax.fori_loop(0, 16, build, 0)

        @pl.when(m == 0)
        def _():
            prepare(1)
            send_tables()

        @pl.when(n < STEPS - 1)
        def _():
            @pl.when(n >= 0)
            def _():
                wait_edges_sent(side)
                wait_rows(ssem.at[side], 127)

            for up in (1, 0):
                ts = jnp.where(side == 0, lax.rem(slab + (1 if up else 31), 32), slab)
                tp = jnp.where(side == 0, plane, lax.rem(plane + (1 if up else 3), 4))
                pltpu.make_async_remote_copy(
                    src_ref=v_ref.at[side, nxt, 3 if up else 0], dst_ref=hb_ref.at[side, nslot, 1 - up],
                    send_sem=hssem.at[side], recv_sem=hrsem.at[side, nslot],
                    device_id=(ts, tp), device_id_type=MESH,
                ).start()

            @pl.when(side == 0)
            def _():
                for up in (1, 0):
                    pltpu.make_async_remote_copy(
                        src_ref=v_ref.at[0, nxt, :, pl.ds(15 if up else 0, 1)],
                        dst_ref=hy_ref.at[nslot, 1 - up, :, pl.ds(0, 1)],
                        send_sem=hssem.at[2], recv_sem=hrsem.at[2, nslot],
                        device_id=(slab, lax.rem(plane + (1 if up else 3), 4)), device_id_type=MESH,
                    ).start()

            gather(side, v_ref[side, nxt].reshape(64, 128), nxt, send_row)

        @pl.when(m == 1)
        def _():
            prepare(0)

        return carry

    lax.fori_loop(0, 2 * STEPS + 2, act, 0)
    wait_rows(s0sem, 127)
    for side in range(2):
        wait_rows(ssem.at[side], 127)
        wait_tiles(hssem.at[side])
    wait_lines(hssem.at[2])
    out_ref[0] = v_ref[0, STEPS % 2]
    out_ref[1] = v_ref[1, STEPS % 2]


def unpack(in_ref, to_ref, fo_ref):
    to_ref[...] = in_ref[0]
    for t in range(4):
        fo_ref[:, t * 128:(t + 1) * 128] = in_ref[1, t]


def body(
    tissue_v, tissue_gates, tissue_diff, fibre_v, fibre_gates, fibre_diff,
    gate_half, gate_rate, gate_cond, gate_rev, junc_cond,
    junc_fibre, junc_fcell, junc_owner, junc_tcell, junc_class,
):
    vmem = pl.BlockSpec(memory_space=pltpu.VMEM)
    anywhere = pl.BlockSpec(memory_space=pl.ANY)
    junctions = [a.reshape(32, 128) for a in (junc_fibre, junc_fcell, junc_owner[:, 0], junc_tcell, junc_class)]
    dma = pltpu.SemaphoreType.DMA
    codes = np.array([[a * 32 + b * 8 + c * 4 + d] * 128 for a, b, c, d in RANKS], np.int32)
    held = pl.pallas_call(
        kernel,
        out_shape=jax.ShapeDtypeStruct((2, 4, 16, 128), f32),
        in_specs=[anywhere] * 17,
        out_specs=vmem,
        scratch_shapes=[pltpu.SMEM((40,), f32)] * 4 + [pltpu.SMEM((8,), f32)] + [pltpu.VMEM((32, 128), i32)] * 5 + [
            pltpu.VMEM((128, 128), i32),
            pltpu.VMEM((2, 2, 4, 16, 128), f32),
            pltpu.VMEM((2, 4, 16, 128), f32),
            pltpu.VMEM((2, 40, 4, 16, 128), f32),
            pltpu.SMEM((240,), f32),
            pltpu.VMEM((128, 4096), bf16),
            pltpu.VMEM((384, 4096), bf16),
            pltpu.VMEM((2, 64, 64, 128), bf16),
            pltpu.VMEM((2, 128, 8192), bf16),
            pltpu.VMEM((2, 8192, 128), bf16),
            pltpu.VMEM((2, 64, 128), i32),
            pltpu.VMEM((2, 64, 128), i32),
            pltpu.VMEM((2, 64, 128), f32),
            pltpu.VMEM((2, 64, 128), f32),
            pltpu.VMEM((3, 64, 128), f32),
            pltpu.VMEM((128, 128), f32),
            pltpu.VMEM((128, 128), f32),
            pltpu.VMEM((2, 64, 128), f32),
            pltpu.VMEM((2, 2, 128, 128), f32),
            pltpu.VMEM((2, 4, 2, 16, 128), f32),
            pltpu.VMEM((4, 2, 4, 8, 128), f32),
            dma((5,)), dma, dma, dma((2,)), dma((2, 2, 3)), dma((3,)), dma((3, 4)), dma((21,)),
        ],
        compiler_params=pltpu.CompilerParams(collective_id=0, has_side_effects=True),
    )(
        tissue_v, tissue_diff, fibre_v, fibre_diff, tissue_gates, fibre_gates,
        gate_half, gate_rate, gate_cond, gate_rev, junc_cond, *junctions, codes,
    )
    return pl.pallas_call(
        unpack,
        out_shape=(jax.ShapeDtypeStruct((4, 16, 128), f32), jax.ShapeDtypeStruct((16, 512), f32)),
        in_specs=[vmem],
        out_specs=(vmem, vmem),
    )(held)


def solution(mesh):
    both = P(("slab", "plane"))
    in_specs = (
        P("slab", "plane", None), P(None, "slab", "plane", None), P("slab", "plane", None),
        P("slab", "plane"), P(None, "slab", "plane"), P("slab", "plane"),
        P(), P(), P(), P(), P(), both, both, P(("slab", "plane"), None), both, both,
    )
    out_specs = (P("slab", "plane", None), P("slab", "plane"))
    return jax.shard_map(body, mesh=mesh, in_specs=in_specs, out_specs=out_specs, check_vma=False)
```

```python
import jax
import jax.numpy as jnp
import numpy as np
from jax import lax
from jax.experimental import pallas as pl
from jax.experimental.pallas import tpu as pltpu
from jax.sharding import PartitionSpec as P

STEPS = 14
DT = 0.1
CUTS = (0, 64)
GROUPS = (0,)
LOG2E = 1.4426950408889634
MESH = pl.DeviceIdType.MESH
f32, bf16, i32 = jnp.float32, jnp.bfloat16, jnp.int32


def rank_table():
    ring = lambda d: min(d, 4 - d)
    every = [(a, b, c, d) for a in range(4) for b in range(4) for c in range(2) for d in range(4)]
    far = lambda o: ring(o[0]) + ring(o[1]) + ring(o[3]) + 0.1 * o[2]
    streams, seen = ([], []), set()
    for o in sorted(every, key=lambda o: -far(o)):
        if o in seen:
            continue
        group = [o] if negative(o) == o else [o, negative(o)]
        seen.update(group)
        to = 0 if len(streams[0]) <= len(streams[1]) else 1
        if len(streams[to]) + len(group) > 64:
            to = 1 - to
        streams[to].extend(group)
    return streams[0] + streams[1]


def negative(o):
    return (-o[0] % 4, -o[1] % 4, o[2], -o[3] % 4)


RANKS = rank_table()
RANK_OF = {o: r for r, o in enumerate(RANKS)}
HERE = RANK_OF[(0, 0, 0, 0)]


def iota(shape, dim):
    return lax.broadcasted_iota(i32, shape, dim)


def kernel(
    tv_ref, td_ref, fv_ref, fd_ref, tg_ref, fg_ref,
    half_in, rate_in, cond_in, rev_in, jcond_in,
    jf_in, jc_in, jo_in, jt_in, jk_in, code_in,
    out_ref,
    half_ref, rate_ref, cond_ref, rev_ref, jcond_ref,
    jf_ref, jc_ref, jo_ref, jt_ref, jk_ref, code_ref,
    v_ref, d_ref, y_ref, prm_ref,
    oht_ref, kv_ref, rmask_ref, ct_ref, c_ref,
    row_ref, lane_ref, gain_ref, gsum_ref, graw_ref,
    s0_ref, r0_ref, s_ref, r_ref, hb_ref, hy_ref,
    gsem, s0sem, r0sem, ssem, rsem, hssem, hrsem, isem,
):
    slab, plane = lax.axis_index("slab"), lax.axis_index("plane")
    z, y, core = slab // 8, lax.rem(slab // 2, 4), lax.rem(slab, 2)
    zs = [lax.rem(z + d, 4) * 8 for d in range(4)]
    ys = [lax.rem(y + d, 4) * 2 for d in range(4)]
    cs = [lax.rem(core + d, 2) for d in range(2)]
    xs = [lax.rem(plane + d, 4) for d in range(4)]

    def device(rank):
        a, b, c, d = RANKS[rank]
        return (zs[a] + ys[b] + cs[c], xs[d])

    peers = sorted((r for r in range(128) if r != HERE), key=lambda r: r % 64)

    barrier = pltpu.get_barrier_semaphore()
    for r in peers:
        pl.semaphore_signal(barrier, inc=1, device_id=device(r), device_id_type=MESH)

    pairs = [
        (jo_in, jo_ref), (code_in, code_ref), (jt_in, jt_ref), (jk_in, jk_ref), (jc_in, jc_ref), (jf_in, jf_ref),
        (jcond_in, jcond_ref), (half_in, half_ref), (rate_in, rate_ref), (cond_in, cond_ref), (rev_in, rev_ref),
        (tv_ref, v_ref.at[0, 0]), (td_ref, d_ref.at[0])]
    for t in range(4):
        pairs.append((fv_ref.at[:, pl.ds(t * 128, 128)], v_ref.at[1, 0, t]))
        pairs.append((fd_ref.at[:, pl.ds(t * 128, 128)], d_ref.at[1, t]))
    arrivals = [pltpu.make_async_copy(a, b, isem.at[k]) for k, (a, b) in enumerate(pairs)]
    loads = [pltpu.make_async_copy(tg_ref, y_ref.at[0], gsem.at[0])]
    for t in range(4):
        loads.append(pltpu.make_async_copy(fg_ref.at[:, :, pl.ds(t * 128, 128)], y_ref.at[1, :, t], gsem.at[1 + t]))
    for copy in arrivals + loads:
        copy.start()
    for copy in arrivals:
        copy.wait()

    def params(k, carry):
        rate, cond = rate_ref[k], cond_ref[k]
        prm_ref[6 * k + 0] = 0.5 * half_ref[k]
        prm_ref[6 * k + 1] = rate * (-1.5 * DT * LOG2E)
        prm_ref[6 * k + 2] = rate * (-0.5 * DT * LOG2E)
        prm_ref[6 * k + 3] = 0.5 * cond
        prm_ref[6 * k + 4] = rev_ref[k]
        prm_ref[6 * k + 5] = cond
        return carry

    lax.fori_loop(0, 40, params, 0)

    sub = iota((128, 128), 0)
    sub64 = iota((64, 128), 0)
    lane = iota((128, 128), 1)
    lane64 = iota((64, 128), 1)
    before = jnp.concatenate([jnp.where(sub < lane, 1.0, 0.0), jnp.ones((128, 128), f32)], axis=1).astype(bf16)

    def chunks(c4, count):
        for u in range(4):
            c = c4 * 4 + u
            at = pl.ds(c, 1)
            cols = pl.ds(pl.multiple_of(c * 128, 128), 128)
            owner = jo_ref[at, :]
            relative = (
                lax.rem(owner // 32 + 4 - z, 4) * 32 + lax.rem(lax.rem(owner // 8, 4) + 4 - y, 4) * 8
                + lax.rem(lax.rem(owner // 4, 2) + 2 - core, 2) * 4 + lax.rem(lax.rem(owner, 4) + 4 - plane, 4))
            hit = code_ref[...] == jnp.broadcast_to(relative, (128, 128))
            onehot = jnp.where(hit, 1.0, 0.0).astype(bf16)
            oht_ref[:, cols] = onehot
            seen = jnp.dot(onehot, before, preferred_element_type=f32)
            rank = jnp.sum(jnp.where(hit, seen[:, :128] + count, 0.0), axis=0, keepdims=True).astype(i32)
            place = sub64 == jnp.broadcast_to(rank, (64, 128))
            cell, fcell = jt_ref[at, :], jc_ref[at, :]
            planes = (
                cell // 128, jk_ref[at, :] + 1, lax.rem(cell, 128), jnp.zeros_like(cell),
                (fcell // 128) * 16 + jf_ref[at, :], lax.rem(fcell, 128))
            for p, value in enumerate(planes):
                value = jnp.broadcast_to(value.astype(f32), (64, 128))
                kv_ref[p * 64:(p + 1) * 64, cols] = jnp.where(place, value, 0.0).astype(bf16)
            count = count + seen[:, 128:]
        return count

    lax.fori_loop(0, 8, chunks, jnp.zeros((128, 128), f32))
    slots = lax.dot_general(oht_ref[...], kv_ref[...], (((1,), (1,)), ((), ())), preferred_element_type=f32)
    first, second, third = slots[:, :128], slots[:, 128:256], slots[:, 256:]
    gain = jnp.zeros((128, 128), f32)
    for k in range(8):
        gain = jnp.where(first == float(k + 1), jcond_ref[k], gain)
    s0_ref[...] = jnp.where(lane < 64, first * 128.0 + second, gain)

    def turn(array):
        return pltpu.roll(array, 64, 1)

    def low_pair(array):
        return jnp.where(lane64 < 64, array[:64], turn(array[64:]))

    def high_pair(array):
        return jnp.where(lane64 < 64, turn(array[:64]), array[64:])

    row_ref[1] = low_pair(third).astype(i32)
    lane_ref[1] = high_pair(third).astype(i32)
    gain_ref[1] = high_pair(s0_ref[...])
    gain_ref[0] = jnp.ones((64, 128), f32)
    graw_ref[1] = gain_ref[1]

    def send_tables():
        pl.semaphore_wait(barrier, 127)
        for r in peers:
            pltpu.make_async_remote_copy(
                src_ref=s0_ref.at[pl.ds(r, 1)], dst_ref=r0_ref.at[pl.ds(RANK_OF[negative(RANKS[r])], 1)],
                send_sem=s0sem, recv_sem=r0sem, device_id=device(r), device_id_type=MESH,
            ).start()
        r0_ref[HERE:HERE + 1, :] = s0_ref[HERE:HERE + 1, :]

    def send_row(side, nxt, i):
        for r in (i, i + 64):
            if r == HERE:
                r_ref[1 - side, nxt, HERE:HERE + 1, :] = s_ref[side, i:i + 1, :]
                continue
            to = RANK_OF[negative(RANKS[r])]
            pltpu.make_async_remote_copy(
                src_ref=s_ref.at[side, pl.ds(i, 1)], dst_ref=r_ref.at[1 - side, nxt, pl.ds(to, 1)],
                send_sem=ssem.at[side], recv_sem=rsem.at[1 - side, nxt, sum(to % 64 < g for g in GROUPS)],
                device_id=device(r), device_id_type=MESH,
            ).start()

    def scatter(side, x, first, total):
        hi = x.astype(bf16)
        lo = (x - hi.astype(f32)).astype(bf16)
        for t in range(0, x.shape[0], 2):
            parts = []
            for i in (t, t + 1):
                m = rmask_ref[side, first + i]
                parts.append(jnp.concatenate(
                    [m * jnp.broadcast_to(hi[i:i + 1], (64, 128)), m * jnp.broadcast_to(lo[i:i + 1], (64, 128))], axis=0))
            at = (first + t) * 128
            total = total + jnp.dot(
                jnp.concatenate(parts, axis=1), c_ref[side, at:at + 256, :], preferred_element_type=f32)
        return total

    def gather(side, v, nxt, send):
        hi = v.astype(bf16)
        lo = (v - hi.astype(f32)).astype(bf16)
        lhs = jnp.concatenate([hi, lo], axis=0)
        for start, stop in zip(CUTS, CUTS[1:]):
            for t in range(start // 2, stop // 2):
                p = jnp.dot(lhs, ct_ref[side, :, t * 256:(t + 1) * 256], preferred_element_type=f32)
                p = p[:64] + p[64:]
                for u in range(2):
                    i = 2 * t + u
                    read = jnp.sum(p[:, u * 128:(u + 1) * 128] * rmask_ref[side, i].astype(f32), axis=0, keepdims=True)
                    s_ref[side, i:i + 1, :] = read * gain_ref[side, i:i + 1, :]
            for i in range(start, stop):
                send(side, nxt, i)

    def received(side, par, low, high):
        a = r_ref[side, par, low:high, :]
        b = r_ref[side, par, 64 + low:64 + high, :]
        return jnp.where(lane64[:high - low] < 64, a, b) * gain_ref[side, low:high, :]

    def membrane(side, par):
        out = []
        for h in range(2):
            v = v_ref[side, par, 2 * h:2 * h + 2].reshape(32, 128)
            vh = 0.5 * v

            def some(j, sums):
                conduct, driven = sums
                for u in range(8):
                    k = 8 * j + u
                    w = vh - prm_ref[6 * k]
                    factor = jnp.exp2(prm_ref[6 * k + 1] + prm_ref[6 * k + 2] * jnp.tanh(w))
                    hc = prm_ref[6 * k + 3]
                    swing = hc * jnp.tanh(w + w)
                    steady = hc + swing if u % 2 == 0 else hc - swing
                    old = y_ref[side, k, 2 * h:2 * h + 2].reshape(32, 128)
                    new = steady + (old - steady) * factor
                    y_ref[side, k, 2 * h:2 * h + 2] = new.reshape(2, 16, 128)
                    conduct = conduct + new
                    driven = driven + prm_ref[6 * k + 4] * new
                return conduct, driven

            zero = jnp.zeros((32, 128), f32)
            conduct, driven = lax.fori_loop(0, 5, some, (zero, zero))
            out.append(v * conduct - driven)
        return jnp.concatenate(out, axis=0)

    row16 = iota((16, 128), 0)
    lane16 = iota((16, 128), 1)

    def tissue_inner(par):
        tiles = [v_ref[0, par, t] for t in range(4)]
        around = [jnp.zeros((16, 128), f32)] + tiles + [jnp.zeros((16, 128), f32)]
        out = []
        for t in range(4):
            here = tiles[t]
            total = around[t] + around[t + 2]
            total = total + jnp.where(row16 == 0, 0.0, pltpu.roll(here, 1, 0))
            total = total + jnp.where(row16 == 15, 0.0, pltpu.roll(here, 15, 0))
            total = total + jnp.where(lane16 == 0, here, pltpu.roll(here, 1, 1))
            total = total + jnp.where(lane16 == 127, here, pltpu.roll(here, 127, 1))
            out.append(total - 6.0 * here)
        return jnp.concatenate(out, axis=0)

    def tissue_outer(par, slot):
        tiles = [v_ref[0, par, t] for t in range(4)]
        out = []
        for t in range(4):
            here = tiles[t]
            ylo = jnp.where(plane == 0, here[0:1], hy_ref[slot, 0, t, 0:1, :])
            yhi = jnp.where(plane == 3, here[15:16], hy_ref[slot, 1, t, 0:1, :])
            out.append(jnp.where(row16 == 0, jnp.broadcast_to(ylo, (16, 128)), 0.0)
                       + jnp.where(row16 == 15, jnp.broadcast_to(yhi, (16, 128)), 0.0))
        out[0] = out[0] + jnp.where(slab == 0, tiles[0], hb_ref[0, slot, 0])
        out[3] = out[3] + jnp.where(slab == 31, tiles[3], hb_ref[0, slot, 1])
        return jnp.concatenate(out, axis=0)

    def fibre_inner(par):
        tiles = [v_ref[1, par, t] for t in range(4)]
        right = [jnp.zeros((16, 128), f32)] + [pltpu.roll(a, 1, 1) for a in tiles]
        left = [pltpu.roll(a, 127, 1) for a in tiles] + [jnp.zeros((16, 128), f32)]
        out = []
        for t in range(4):
            total = jnp.where(lane16 == 0, right[t], right[t + 1])
            total = total + jnp.where(lane16 == 127, left[t + 1], left[t])
            out.append(total - 2.0 * tiles[t])
        return jnp.concatenate(out, axis=0)

    def fibre_outer(par, slot):
        right = jnp.where(plane == 0, v_ref[1, par, 0], pltpu.roll(hb_ref[1, slot, 0], 1, 1))
        left = jnp.where(plane == 3, v_ref[1, par, 3], pltpu.roll(hb_ref[1, slot, 1], 127, 1))
        none = jnp.zeros((16, 128), f32)
        return jnp.concatenate(
            [jnp.where(lane16 == 0, right, 0.0), none, none, jnp.where(lane16 == 127, left, 0.0)], axis=0)

    def wait_rows(sem, rows):
        pltpu.make_async_copy(r0_ref.at[pl.ds(0, rows)], r0_ref.at[pl.ds(0, rows)], sem).wait()

    def wait_tiles(sem):
        pltpu.make_async_copy(hb_ref.at[0, 0], hb_ref.at[0, 0], sem).wait()

    def wait_lines(sem):
        pltpu.make_async_copy(hy_ref.at[0, :, :, pl.ds(0, 1)], hy_ref.at[0, :, :, pl.ds(0, 1)], sem).wait()

    def wait_edges_sent(side):
        wait_tiles(hssem.at[side])

        @pl.when(side == 0)
        def _():
            wait_lines(hssem.at[2])

    def prepare(side):
        def flip(i8, carry):
            for u in range(8):
                i = i8 * 8 + u
                here = jnp.where(
                    sub == jnp.broadcast_to(lane_ref[side, pl.ds(i, 1), :], (128, 128)), 1.0, 0.0)
                c_ref[side, pl.ds(pl.multiple_of(i * 128, 128), 128), :] = here.T.astype(bf16)
            return carry

        lax.fori_loop(0, 8, flip, 0)
        total = scatter(side, graw_ref[side], 0, jnp.zeros((128, 128), f32))
        gsum_ref[side] = total[:64] + total[64:]
        for copy in loads[:1] if side == 0 else loads[1:]:
            copy.wait()

        def scale(k, carry):
            y_ref[side, k] = y_ref[side, k] * prm_ref[6 * k + 5]
            return carry

        lax.fori_loop(0, 40, scale, 0)

    def act(m, carry):
        n = m // 2 - 1
        side = lax.rem(lax.rem(m, 2) + n + 2, 2)
        other = 1 - side
        par, slot = lax.rem(n + 2, 2), lax.rem(n + 4, 4)
        nxt, nslot = 1 - par, lax.rem(n + 5, 4)

        @pl.when(n >= 0)
        def _():
            v = v_ref[side, par].reshape(64, 128)
            graw_ref[2] = v - DT * (membrane(side, par) + gsum_ref[side] * v)
            diffusion = d_ref[side].reshape(64, 128)

            @pl.when(side == 0)
            def _():
                graw_ref[2] = graw_ref[2] + DT * diffusion * tissue_inner(par)

            @pl.when(side == 1)
            def _():
                graw_ref[2] = graw_ref[2] + DT * diffusion * fibre_inner(par)

            total, high = jnp.zeros((128, 128), f32), 64
            for g, low in enumerate(GROUPS):
                wait_rows(rsem.at[side, par, g], 2 * (high - low) - (low <= HERE % 64 < high))
                total = scatter(side, received(side, par, low, high), low, total)
                high = low
            known = graw_ref[2] + DT * (total[:64] + total[64:])
            wait_tiles(hrsem.at[side, slot])

            @pl.when(side == 0)
            def _():
                wait_lines(hrsem.at[2, slot])
                v_ref[0, nxt] = (known + DT * diffusion * tissue_outer(par, slot)).reshape(4, 16, 128)

            @pl.when(side == 1)
            def _():
                v_ref[1, nxt] = (known + DT * diffusion * fibre_outer(par, slot)).reshape(4, 16, 128)

        @pl.when(n < 0)
        def _():
            @pl.when(side == 0)
            def _():
                wait_rows(r0sem, 127)
                table = r0_ref[...]
                cell = low_pair(table).astype(i32)
                row_ref[0] = cell // 128
                lane_ref[0] = lax.rem(cell, 128)
                graw_ref[0] = high_pair(table)

            def build(i4, carry):
                for u in range(4):
                    i = i4 * 4 + u
                    at = pl.ds(i, 1)
                    cols = pl.ds(pl.multiple_of(i * 128, 128), 128)
                    rmask_ref[side, i] = jnp.where(
                        sub64 == jnp.broadcast_to(row_ref[side, at, :], (64, 128)), 1.0, 0.0).astype(bf16)
                    ct_ref[side, :, cols] = jnp.where(
                        sub == jnp.broadcast_to(lane_ref[side, at, :], (128, 128)), 1.0, 0.0).astype(bf16)
                return carry

            lax.fori_loop(0, 16, build, 0)

        @pl.when(m == 0)
        def _():
            send_tables()

        @pl.when(n < STEPS - 1)
        def _():
            @pl.when(n >= 0)
            def _():
                wait_edges_sent(side)
                wait_rows(ssem.at[side], 127)

            for up in (1, 0):
                ts = jnp.where(side == 0, lax.rem(slab + (1 if up else 31), 32), slab)
                tp = jnp.where(side == 0, plane, lax.rem(plane + (1 if up else 3), 4))
                pltpu.make_async_remote_copy(
                    src_ref=v_ref.at[side, nxt, 3 if up else 0], dst_ref=hb_ref.at[side, nslot, 1 - up],
                    send_sem=hssem.at[side], recv_sem=hrsem.at[side, nslot],
                    device_id=(ts, tp), device_id_type=MESH,
                ).start()

            @pl.when(side == 0)
            def _():
                for up in (1, 0):
                    pltpu.make_async_remote_copy(
                        src_ref=v_ref.at[0, nxt, :, pl.ds(15 if up else 0, 1)],
                        dst_ref=hy_ref.at[nslot, 1 - up, :, pl.ds(0, 1)],
                        send_sem=hssem.at[2], recv_sem=hrsem.at[2, nslot],
                        device_id=(slab, lax.rem(plane + (1 if up else 3), 4)), device_id_type=MESH,
                    ).start()

            gather(side, v_ref[side, nxt].reshape(64, 128), nxt, send_row)

        @pl.when(m == 0)
        def _():
            prepare(1)

        @pl.when(m == 1)
        def _():
            prepare(0)

        return carry

    lax.fori_loop(0, 2 * STEPS + 2, act, 0)
    wait_rows(s0sem, 127)
    for side in range(2):
        wait_rows(ssem.at[side], 127)
        wait_tiles(hssem.at[side])
    wait_lines(hssem.at[2])
    out_ref[0] = v_ref[0, STEPS % 2]
    out_ref[1] = v_ref[1, STEPS % 2]


def unpack(in_ref, to_ref, fo_ref):
    to_ref[...] = in_ref[0]
    for t in range(4):
        fo_ref[:, t * 128:(t + 1) * 128] = in_ref[1, t]


def body(
    tissue_v, tissue_gates, tissue_diff, fibre_v, fibre_gates, fibre_diff,
    gate_half, gate_rate, gate_cond, gate_rev, junc_cond,
    junc_fibre, junc_fcell, junc_owner, junc_tcell, junc_class,
):
    vmem = pl.BlockSpec(memory_space=pltpu.VMEM)
    anywhere = pl.BlockSpec(memory_space=pl.ANY)
    junctions = [a.reshape(32, 128) for a in (junc_fibre, junc_fcell, junc_owner[:, 0], junc_tcell, junc_class)]
    dma = pltpu.SemaphoreType.DMA
    codes = np.array([[a * 32 + b * 8 + c * 4 + d] * 128 for a, b, c, d in RANKS], np.int32)
    held = pl.pallas_call(
        kernel,
        out_shape=jax.ShapeDtypeStruct((2, 4, 16, 128), f32),
        in_specs=[anywhere] * 17,
        out_specs=vmem,
        scratch_shapes=[pltpu.SMEM((40,), f32)] * 4 + [pltpu.SMEM((8,), f32)] + [pltpu.VMEM((32, 128), i32)] * 5 + [
            pltpu.VMEM((128, 128), i32),
            pltpu.VMEM((2, 2, 4, 16, 128), f32),
            pltpu.VMEM((2, 4, 16, 128), f32),
            pltpu.VMEM((2, 40, 4, 16, 128), f32),
            pltpu.SMEM((240,), f32),
            pltpu.VMEM((128, 4096), bf16),
            pltpu.VMEM((384, 4096), bf16),
            pltpu.VMEM((2, 64, 64, 128), bf16),
            pltpu.VMEM((2, 128, 8192), bf16),
            pltpu.VMEM((2, 8192, 128), bf16),
            pltpu.VMEM((2, 64, 128), i32),
            pltpu.VMEM((2, 64, 128), i32),
            pltpu.VMEM((2, 64, 128), f32),
            pltpu.VMEM((2, 64, 128), f32),
            pltpu.VMEM((3, 64, 128), f32),
            pltpu.VMEM((128, 128), f32),
            pltpu.VMEM((128, 128), f32),
            pltpu.VMEM((2, 64, 128), f32),
            pltpu.VMEM((2, 2, 128, 128), f32),
            pltpu.VMEM((2, 4, 2, 16, 128), f32),
            pltpu.VMEM((4, 2, 4, 8, 128), f32),
            dma((5,)), dma, dma, dma((2,)), dma((2, 2, 3)), dma((3,)), dma((3, 4)), dma((21,)),
        ],
        compiler_params=pltpu.CompilerParams(collective_id=0, has_side_effects=True),
    )(
        tissue_v, tissue_diff, fibre_v, fibre_diff, tissue_gates, fibre_gates,
        gate_half, gate_rate, gate_cond, gate_rev, junc_cond, *junctions, codes,
    )
    return pl.pallas_call(
        unpack,
        out_shape=(jax.ShapeDtypeStruct((4, 16, 128), f32), jax.ShapeDtypeStruct((16, 512), f32)),
        in_specs=[vmem],
        out_specs=(vmem, vmem),
    )(held)


def solution(mesh):
    both = P(("slab", "plane"))
    in_specs = (
        P("slab", "plane", None), P(None, "slab", "plane", None), P("slab", "plane", None),
        P("slab", "plane"), P(None, "slab", "plane"), P("slab", "plane"),
        P(), P(), P(), P(), P(), both, both, P(("slab", "plane"), None), both, both,
    )
    out_specs = (P("slab", "plane", None), P("slab", "plane"))
    return jax.shard_map(body, mesh=mesh, in_specs=in_specs, out_specs=out_specs, check_vma=False)
```
